8 devices in a mesh: ens: 1 (over z), col: 2 (over y), row: 4 (over x, core).
Axes of the slice: x: 2, y: 2, z: 1, core: 2. Of those that a mesh axis runs over, the one named last changes fastest.
Arguments:
- u_init: float32 [2048, 2048], P(('ens', 'row'), 'col')
- v_init: float32 [2048, 2048], P(('ens', 'row'), 'col')
- stencil_w: float32 [64, 3, 3], replicated
Outputs:
- output 1: float32 [2048, 2048], P(('ens', 'row'), 'col')
- output 2: float32 [2048, 2048], P(('ens', 'row'), 'col')
All inputs are finite; a program needn't handle non-finite values.
Results may differ from the reference program's by a relative error of at most 0.001.
Values are sent between devices in bfloat16 or wider.
A program may use at most 1 GiB of HBM per device.

```python
import jax
import jax.numpy as jnp
from jax import lax

GRID_ROWS = 2048
GRID_COLS = 2048
NUM_STEPS = 64
TIME_STEP = 0.5


def block_field(base_key, block_rows, block_cols):
    block_vals = jax.random.normal(base_key, (GRID_ROWS // block_rows, GRID_COLS // block_cols), jnp.float32)
    spread = jnp.broadcast_to(block_vals[:, None, :, None], (GRID_ROWS // block_rows, block_rows, GRID_COLS // block_cols, block_cols))
    return spread.reshape(GRID_ROWS, GRID_COLS)


def setup_inputs(seed: int = 0, part: int = 0) -> dict:
    part_key = jax.random.fold_in(jax.random.key(seed), part)
    key_ublock, key_unoise, key_vblock, key_vnoise = jax.random.split(part_key, 4)
    u_init = block_field(key_ublock, 8, 8) + 0.3 * jax.random.normal(key_unoise, (GRID_ROWS, GRID_COLS), jnp.float32)
    v_init = 0.5 * block_field(key_vblock, 8, 8) + 0.2 * jax.random.normal(key_vnoise, (GRID_ROWS, GRID_COLS), jnp.float32)
    key_pair, key_centre, key_total = jax.random.split(jax.random.key(seed + 1), 3)
    pair_weights = jax.random.uniform(key_pair, (NUM_STEPS, 4), jnp.float32, minval=0.07, maxval=0.13)
    centre = jax.random.uniform(key_centre, (NUM_STEPS,), jnp.float32, minval=0.2, maxval=0.35)
    weight_total = jax.random.uniform(key_total, (NUM_STEPS,), jnp.float32, minval=0.93, maxval=0.98)
    raw_weights = jnp.stack([
        pair_weights[:, 2], pair_weights[:, 0], pair_weights[:, 3],
        pair_weights[:, 1], centre, pair_weights[:, 1],
        pair_weights[:, 3], pair_weights[:, 0], pair_weights[:, 2]], axis=1)
    weight_scale = weight_total / jnp.sum(raw_weights, axis=1)
    stencil_w = (raw_weights * weight_scale[:, None]).reshape(NUM_STEPS, 3, 3)
    return {"u_init": u_init, "v_init": v_init, "stencil_w": stencil_w}


def stencil_sum(field_now, step_w):
    total_acc = step_w[0, 0] * jnp.roll(field_now, (1, 1), axis=(0, 1))
    for tap_index in range(1, 9):
        row_off, col_off = divmod(tap_index, 3)
        total_acc = total_acc + step_w[row_off, col_off] * jnp.roll(field_now, (1 - row_off, 1 - col_off), axis=(0, 1))
    return total_acc


def reference(u_init, v_init, stencil_w):
    def one_step(state_pair, step_w):
        u_now, v_now = state_pair
        v_next = v_now + (stencil_sum(u_now, step_w) - u_now)
        u_next = u_now + TIME_STEP * v_next
        return (u_next, v_next), None

    (u_final, v_final), _ = lax.scan(one_step, (u_init, v_init), stencil_w)
    return (u_final, v_final)
```

```python
import functools

import jax
import jax.numpy as jnp
from jax import lax
from jax.experimental import pallas as pl
from jax.experimental.pallas import tpu as pltpu
from jax.sharding import PartitionSpec as P

HALO = 16
CHUNK = 13
NC = 9
NB = 11
SCALE = 0.125
MESH = pl.DeviceIdType.MESH


def kernel(steps, rows, cols, halo, chunk, w_ref, u_hbm, v_hbm, uo_hbm, vo_hbm,
           raw, gsend, state_a, state_b, wide, edge, sbuf, rbuf,
           load_sem, col_sems, row_sems, diag_sems, send_sems, recv_sems, out_sem):
    R = (rows + 2 * halo) // 8
    nblk = cols // 128
    n_row = lax.axis_size("row")
    me_row, me_col = lax.axis_index("row"), lax.axis_index("col")
    up, down = lax.rem(me_row + n_row - 1, n_row), lax.rem(me_row + 1, n_row)
    other = 1 - me_col

    loads = []
    for f, src in enumerate((u_hbm, v_hbm)):
        for b in (0, nblk - 1, *range(1, nblk - 1)):
            cp = pltpu.make_async_copy(src.at[:, pl.ds(b * 128, 128)],
                                       raw.at[f, b, pl.ds(halo, rows), :], load_sem.at[f, b])
            cp.start()
            loads.append(cp)

    barrier = pltpu.get_barrier_semaphore()
    peers = [(up, me_col), (down, me_col), (me_row, other), (up, other), (down, other)]
    for r, c in peers:
        pl.semaphore_signal(barrier, inc=1, device_id={"row": r, "col": c}, device_id_type=MESH)
    pl.semaphore_wait(barrier, len(peers))

    states = (state_a, state_b)
    lane = lax.broadcasted_iota(jnp.int32, (8, 128), 1)

    def remote(src, dst, sems, r, c):
        cp = pltpu.make_async_remote_copy(src_ref=src, dst_ref=dst, send_sem=sems.at[0], recv_sem=sems.at[1],
                                          device_id={"row": r, "col": c}, device_id_type=MESH)
        cp.start()
        return cp

    first = [[], []]
    for f in range(2):
        mine = loads[f * nblk:(f + 1) * nblk]
        mine[0].wait()
        mine[1].wait()

        def build(i, _, f=f):
            for q in range(8):
                at = pl.multiple_of(i * 64 + q * 8, 8)
                gsend[f, pl.ds(at, 8), :] = jnp.where(lane < 64, raw[f, 0, pl.ds(halo + at, 8), :],
                                                      raw[f, nblk - 1, pl.ds(halo + at, 8), :])
            return 0
        lax.fori_loop(0, rows // 64, build, 0)
        first[f].append(remote(gsend.at[f], raw.at[f, nblk, pl.ds(halo, rows), :], col_sems.at[f], me_row, other))
        first[f].append(remote(gsend.at[f, pl.ds(0, halo), :], raw.at[f, nblk, pl.ds(halo + rows, halo), :],
                               diag_sems.at[f, 0], up, other))
        first[f].append(remote(gsend.at[f, pl.ds(rows - halo, halo), :], raw.at[f, nblk, pl.ds(0, halo), :],
                               diag_sems.at[f, 1], down, other))
        for cp in mine[2:]:
            cp.wait()
        first[f].append(remote(raw.at[f, pl.ds(0, nblk), pl.ds(halo, halo), :],
                               raw.at[f, pl.ds(0, nblk), pl.ds(halo + rows, halo), :], row_sems.at[f, 0], up, me_col))
        first[f].append(remote(raw.at[f, pl.ds(0, nblk), pl.ds(rows, halo), :],
                               raw.at[f, pl.ds(0, nblk), pl.ds(0, halo), :], row_sems.at[f, 1], down, me_col))

    groups = -(-R // 16)

    def reg(r, c):
        return pl.ds(pl.multiple_of((r * NB + c) * 8, 8), 8)

    for f in range(2):
        for cp in first[f]:
            cp.wait()

        def group(i, _, f=f):
            r0 = i * (R - 16) // (groups - 1)
            for b in range(NC):
                parts = []
                for q in range(16):
                    x = raw[0, b, pl.ds(r0 + q, 8, stride=R), :]
                    if f == 1:
                        x = x - 0.5 * raw[1, b, pl.ds(r0 + q, 8, stride=R), :]
                    parts.append(x * SCALE)
                wide[pl.ds(b * 128, 128), :] = jnp.concatenate(parts, axis=0).T
            for c in range(NC):
                back = wide[pl.ds(c, 128, stride=NC), :].T
                for q in range(16):
                    x = back[q * 8:q * 8 + 8, :]
                    states[f][reg(r0 + q, c), :] = x
                    if c == 0:
                        states[f][reg(r0 + q, 10), :] = pltpu.roll(x, 127, 1)
                    if c == NC - 1:
                        states[f][reg(r0 + q, 9), :] = pltpu.roll(x, 1, 1)
            return 0
        lax.fori_loop(0, groups, group, 0)

    def level(t, cur, new):
        w00, w01, w02, w10, w11 = (w_ref[t, 0, 0], w_ref[t, 0, 1], w_ref[t, 0, 2], w_ref[t, 1, 0], w_ref[t, 1, 1])
        splat = lambda x: jnp.full((8, 128), x, jnp.float32)
        alpha, beta = splat(0.25 * (w00 + w02)), splat(0.25 * (w02 - w00))
        side, mid_s, centre = splat(0.5 * w01), splat(0.5 * w10), splat(1.5 + 0.5 * w11)

        def contrib(r, want="TMB"):
            u = [cur[reg(r, c), :] for c in range(NB)]
            above, mid, below = [], [], []
            for c in range(NC):
                left = u[c - 1] if c else u[9]
                right = u[c + 1] if c < NC - 1 else u[10]
                s, d = left + right, right - left
                e, bd = alpha * s + side * u[c], beta * d
                above.append(e + bd)
                if "M" in want:
                    mid.append(mid_s * s + centre * u[c])
                    below.append(e - bd)
            return above, mid, below

        def emit(r, acc, below):
            for c in range(NC):
                x = (acc[c] + below[c]) - new[reg(r, c), :]
                new[reg(r, c), :] = x
                if c == 0:
                    new[reg(r, 10), :] = pltpu.roll(x, 127, 1)
                if c == NC - 1:
                    new[reg(r, 9), :] = pltpu.roll(x, 1, 1)

        last, _, _ = contrib(R - 1, "T")
        above, mid, below = contrib(0)
        for c in range(NC):
            edge[c] = pltpu.roll(below[c], 7, 0)
        acc = [pltpu.roll(last[c], 1, 0) + mid[c] for c in range(NC)]

        def rowstep(r, above, acc):
            nabove, mid, below = contrib(r + 1)
            emit(r, acc, below)
            return nabove, [above[c] + mid[c] for c in range(NC)]

        def body(it, carry):
            above, acc = carry
            for q in range(chunk):
                above, acc = rowstep(it * chunk + q, above, acc)
            return above, acc

        trips = (R - 1) // chunk
        above, acc = lax.fori_loop(0, trips, body, (above, acc))
        for r in range(trips * chunk, R - 1):
            above, acc = rowstep(r, above, acc)
        emit(R - 1, acc, [edge[c] for c in range(NC)])

    def pair(i, _):
        level(2 * i, state_a, state_b)
        level(2 * i + 1, state_b, state_a)
        return 0

    def strided(r, c, s):
        return pl.ds((r * NB + c) * 8 + s, 8, stride=NB * 8)

    def exchange(slot):
        copies = []
        for d, (peer, r0, s) in enumerate(((up, halo, 0), (down, R - 2 * halo, 7))):
            for f in range(2):
                for g in range(halo // 8):
                    for c in range(NB):
                        sbuf[slot, d, f, g, c] = states[f][strided(r0 + 8 * g, c, s), :]
            copies.append(pltpu.make_async_remote_copy(
                src_ref=sbuf.at[slot, d], dst_ref=rbuf.at[slot, d], send_sem=send_sems.at[slot, d],
                recv_sem=recv_sems.at[slot, d], device_id={"row": peer, "col": me_col}, device_id_type=MESH))
            copies[-1].start()
        for d, (r0, s) in enumerate(((R - halo, 7), (0, 0))):
            copies[d].wait()
            for f in range(2):
                for g in range(halo // 8):
                    for c in range(NB):
                        states[f][strided(r0 + 8 * g, c, s), :] = rbuf[slot, d, f, g, c]

    def phase(p, _):
        lax.fori_loop(p * (halo // 2), (p + 1) * (halo // 2), pair, 0)

        @pl.when(p < steps // halo - 1)
        def _():
            exchange(lax.rem(p, 2))
        return 0
    lax.fori_loop(0, steps // halo, phase, 0)

    outs = []
    for f, dst in enumerate((uo_hbm, vo_hbm)):
        def ungroup(i, _, f=f):
            r0 = i * (R - 16) // (groups - 1)
            for c in range(NC):
                parts = []
                for q in range(16):
                    x = state_a[reg(r0 + q, c), :]
                    if f == 1:
                        x = (x - state_b[reg(r0 + q, c), :]) * (2.0 / SCALE)
                    else:
                        x = x * (1.0 / SCALE)
                    parts.append(x)
                wide[pl.ds(c, 128, stride=NC), :] = jnp.concatenate(parts, axis=0).T
            for b in range(nblk):
                back = wide[pl.ds(b * 128, 128), :].T
                for q in range(16):
                    raw[f, b, pl.ds(r0 + q, 8, stride=R), :] = back[q * 8:q * 8 + 8, :]
            return 0
        lax.fori_loop(0, groups, ungroup, 0)
        for b in range(nblk):
            cp = pltpu.make_async_copy(raw.at[f, b, pl.ds(halo, rows), :], dst.at[:, pl.ds(b * 128, 128)],
                                       out_sem.at[f, b])
            cp.start()
            outs.append(cp)
    for cp in outs:
        cp.wait()


def solution(mesh):
    tile_spec = P(("ens", "row"), "col")

    def local_run(u_tile, v_tile, stencil_w):
        rows, cols = u_tile.shape
        steps = stencil_w.shape[0]
        halo = HALO
        R = (rows + 2 * halo) // 8
        nblk = cols // 128
        f32 = jnp.float32
        dma = pltpu.SemaphoreType.DMA
        return pl.pallas_call(
            functools.partial(kernel, steps, rows, cols, halo, CHUNK),
            out_shape=[jax.ShapeDtypeStruct((rows, cols), f32)] * 2,
            in_specs=[pl.BlockSpec(memory_space=pltpu.SMEM)] + [pl.BlockSpec(memory_space=pl.ANY)] * 2,
            out_specs=[pl.BlockSpec(memory_space=pl.ANY)] * 2,
            scratch_shapes=[
                pltpu.VMEM((2, nblk + 1, 8 * R, 128), f32),
                pltpu.VMEM((2, rows, 128), f32),
                pltpu.VMEM((R * NB * 8, 128), f32),
                pltpu.VMEM((R * NB * 8, 128), f32),
                pltpu.VMEM((128 * NC, 128), f32),
                pltpu.VMEM((NC, 8, 128), f32),
                pltpu.VMEM((2, 2, 2, halo // 8, NB, 8, 128), f32),
                pltpu.VMEM((2, 2, 2, halo // 8, NB, 8, 128), f32),
                dma((2, nblk)), dma((2, 2)), dma((2, 2, 2)), dma((2, 2, 2)), dma((2, 2)), dma((2, 2)), dma((2, nblk)),
            ],
            compiler_params=pltpu.CompilerParams(collective_id=0, has_side_effects=True,
                                                 vmem_limit_bytes=48 * 1024 * 1024),
        )(stencil_w, u_tile, v_tile)

    return jax.shard_map(local_run, mesh=mesh, in_specs=(tile_spec, tile_spec, P()), out_specs=(tile_spec, tile_spec), check_vma=False)
```

```python
import functools

import jax
import jax.numpy as jnp
from jax import lax
from jax.experimental import pallas as pl
from jax.experimental.pallas import tpu as pltpu
from jax.sharding import PartitionSpec as P

HALO = 16
CHUNK = 22
ORDER = ((0, 8), (1, 2, 3, 4), (5, 6, 7))
NC = 9
NB = 11
SCALE = 0.125
MESH = pl.DeviceIdType.MESH


def kernel(steps, rows, cols, halo, chunk, w_ref, u_hbm, v_hbm, uo_hbm, vo_hbm,
           raw, gsend, state_a, state_b, wide, sbuf, rbuf,
           load_sem, col_sems, row_sems, diag_sems, send_sems, recv_sems, out_sem):
    R = (rows + 2 * halo) // 8
    nblk = cols // 128
    n_row = lax.axis_size("row")
    me_row, me_col = lax.axis_index("row"), lax.axis_index("col")
    up, down = lax.rem(me_row + n_row - 1, n_row), lax.rem(me_row + 1, n_row)
    other = 1 - me_col

    loads = []
    for f, src in enumerate((u_hbm, v_hbm)):
        for b in (0, nblk - 1, *range(1, nblk - 1)):
            cp = pltpu.make_async_copy(src.at[:, pl.ds(b * 128, 128)],
                                       raw.at[f, b, pl.ds(halo, rows), :], load_sem.at[f, b])
            cp.start()
            loads.append(cp)

    barrier = pltpu.get_barrier_semaphore()
    peers = [(up, me_col), (down, me_col), (me_row, other), (up, other), (down, other)]
    for r, c in peers:
        pl.semaphore_signal(barrier, inc=1, device_id={"row": r, "col": c}, device_id_type=MESH)
    pl.semaphore_wait(barrier, len(peers))

    states = (state_a, state_b)
    lane = lax.broadcasted_iota(jnp.int32, (8, 128), 1)

    def remote(src, dst, sems, r, c):
        cp = pltpu.make_async_remote_copy(src_ref=src, dst_ref=dst, send_sem=sems.at[0], recv_sem=sems.at[1],
                                          device_id={"row": r, "col": c}, device_id_type=MESH)
        cp.start()
        return cp

    first = [[], []]
    for f in range(2):
        mine = loads[f * nblk:(f + 1) * nblk]
        mine[0].wait()
        mine[1].wait()

        def build(i, _, f=f):
            for q in range(8):
                at = pl.multiple_of(i * 64 + q * 8, 8)
                gsend[f, pl.ds(at, 8), :] = jnp.where(lane < 64, raw[f, 0, pl.ds(halo + at, 8), :],
                                                      raw[f, nblk - 1, pl.ds(halo + at, 8), :])
            return 0
        lax.fori_loop(0, rows // 64, build, 0)
        first[f].append(remote(gsend.at[f], raw.at[f, nblk, pl.ds(halo, rows), :], col_sems.at[f], me_row, other))
        first[f].append(remote(gsend.at[f, pl.ds(0, halo), :], raw.at[f, nblk, pl.ds(halo + rows, halo), :],
                               diag_sems.at[f, 0], up, other))
        first[f].append(remote(gsend.at[f, pl.ds(rows - halo, halo), :], raw.at[f, nblk, pl.ds(0, halo), :],
                               diag_sems.at[f, 1], down, other))
        for cp in mine[2:]:
            cp.wait()
        first[f].append(remote(raw.at[f, pl.ds(0, nblk), pl.ds(halo, halo), :],
                               raw.at[f, pl.ds(0, nblk), pl.ds(halo + rows, halo), :], row_sems.at[f, 0], up, me_col))
        first[f].append(remote(raw.at[f, pl.ds(0, nblk), pl.ds(rows, halo), :],
                               raw.at[f, pl.ds(0, nblk), pl.ds(0, halo), :], row_sems.at[f, 1], down, me_col))

    groups = -(-R // 16)

    def reg(r, c):
        return pl.ds(pl.multiple_of((r * NB + c) * 8, 8), 8)

    for f in range(2):
        for cp in first[f]:
            cp.wait()

        def group(i, _, f=f):
            r0 = i * (R - 16) // (groups - 1)
            for b in range(NC):
                parts = []
                for q in range(16):
                    x = raw[0, b, pl.ds(r0 + q, 8, stride=R), :]
                    if f == 1:
                        x = x - 0.5 * raw[1, b, pl.ds(r0 + q, 8, stride=R), :]
                    parts.append(x * SCALE)
                wide[pl.ds(b * 128, 128), :] = jnp.concatenate(parts, axis=0).T
            for c in range(NC):
                back = wide[pl.ds(c, 128, stride=NC), :].T
                for q in range(16):
                    x = back[q * 8:q * 8 + 8, :]
                    states[f][reg(r0 + q, c), :] = x
                    if c == 0:
                        states[f][reg(r0 + q, 10), :] = pltpu.roll(x, 127, 1)
                    if c == NC - 1:
                        states[f][reg(r0 + q, 9), :] = pltpu.roll(x, 1, 1)
            return 0
        lax.fori_loop(0, groups, group, 0)

    def level(t, cur, new):
        w00, w01, w02, w10, w11 = (w_ref[t, 0, 0], w_ref[t, 0, 1], w_ref[t, 0, 2], w_ref[t, 1, 0], w_ref[t, 1, 1])
        splat = lambda x: jnp.full((8, 128), x, jnp.float32)
        alpha, beta = splat(0.25 * (w00 + w02)), splat(0.25 * (w02 - w00))
        side, mid_s, centre = splat(0.5 * w01), splat(0.5 * w10), splat(1.5 + 0.5 * w11)

        def contrib(r, c):
            here = cur[reg(r, c), :]
            left = cur[reg(r, c - 1 if c else 9), :]
            right = cur[reg(r, c + 1 if c < NC - 1 else 10), :]
            s, d = left + right, right - left
            e, bd = alpha * s + side * here, beta * d
            return e + bd, mid_s * s + centre * here, e - bd

        def emit(r, c, acc, below):
            x = (acc + below) - new[reg(r, c), :]
            new[reg(r, c), :] = x
            return x

        def edges(r, c, x):
            if c == 0:
                new[reg(r, 10), :] = pltpu.roll(x, 127, 1)
            if c == NC - 1:
                new[reg(r, 9), :] = pltpu.roll(x, 1, 1)

        lead = (R - 1) % chunk
        carry = []
        for c in range(NC):
            before, _, _ = contrib(R - 2, c)
            last, mid, _ = contrib(R - 1, c)
            above, mid0, below = contrib(0, c)
            emit(R - 1, c, before + mid, pltpu.roll(below, 7, 0))
            acc = pltpu.roll(last, 1, 0) + mid0
            for r in range(lead):
                nabove, mid, below = contrib(r + 1, c)
                emit(r, c, acc, below)
                above, acc = nabove, above + mid
            carry.append((above, acc))

        def body(it, carry):
            carry = list(carry)
            for r in (R - 1, *range(lead)):
                for c in (0, NC - 1):
                    edges(r, c, new[reg(r, c), :])
            for cs in ORDER:
                for q in range(chunk):
                    r = it * chunk + lead + q
                    for c in cs:
                        above, acc = carry[c]
                        nabove, mid, below = contrib(r + 1, c)
                        edges(r, c, emit(r, c, acc, below))
                        carry[c] = nabove, above + mid
            return tuple(carry)

        lax.fori_loop(0, (R - 1) // chunk, body, tuple(carry))

    def strided(r, c, s):
        return pl.ds((r * NB + c) * 8 + s, 8, stride=NB * 8)

    def copies(f, slot):
        return [pltpu.make_async_remote_copy(
            src_ref=sbuf.at[slot, d, f], dst_ref=rbuf.at[slot, d, f], send_sem=send_sems.at[slot, d, f],
            recv_sem=recv_sems.at[slot, d, f], device_id={"row": peer, "col": me_col}, device_id_type=MESH)
            for d, peer in enumerate((up, down))]

    def send(f, slot):
        for d, (r0, s) in enumerate(((halo, 0), (R - 2 * halo, 7))):
            for g in range(halo // 8):
                for c in range(NC):
                    sbuf[slot, d, f, g, c] = states[f][strided(r0 + 8 * g, c, s), :]
        for cp in copies(f, slot):
            cp.start()

    def receive(f, slot):
        for d, (r0, s) in enumerate(((R - halo, 7), (0, 0))):
            copies(f, slot)[d].wait()
            for g in range(halo // 8):
                for c in range(NC):
                    states[f][strided(r0 + 8 * g, c, s), :] = rbuf[slot, d, f, g, c]

        def fix(i, _):
            for r0 in (0, R - halo):
                for q in range(8):
                    r = r0 + i * 8 + q
                    states[f][reg(r, 10), :] = pltpu.roll(states[f][reg(r, 0), :], 127, 1)
                    states[f][reg(r, 9), :] = pltpu.roll(states[f][reg(r, NC - 1), :], 1, 1)
            return 0
        lax.fori_loop(0, halo // 8, fix, 0)

    def pair(i, _):
        level(2 * i, state_a, state_b)
        done = lax.rem(2 * i + 2, halo) == 0
        more = 2 * i + 2 < steps
        slot = lax.rem((2 * i + 2) // halo, 2)

        @pl.when(done & more)
        def _():
            send(1, slot)
        level(2 * i + 1, state_b, state_a)

        @pl.when(done & more)
        def _():
            send(0, slot)
            receive(1, slot)
            receive(0, slot)
        return 0
    lax.fori_loop(0, steps // 2, pair, 0)

    outs = []
    for f, dst in enumerate((uo_hbm, vo_hbm)):
        def ungroup(i, _, f=f):
            r0 = i * (R - 16) // (groups - 1)
            for c in range(NC):
                parts = []
                for q in range(16):
                    x = state_a[reg(r0 + q, c), :]
                    if f == 1:
                        x = (x - state_b[reg(r0 + q, c), :]) * (2.0 / SCALE)
                    else:
                        x = x * (1.0 / SCALE)
                    parts.append(x)
                wide[pl.ds(c, 128, stride=NC), :] = jnp.concatenate(parts, axis=0).T
            for b in range(nblk):
                back = wide[pl.ds(b * 128, 128), :].T
                for q in range(16):
                    raw[f, b, pl.ds(r0 + q, 8, stride=R), :] = back[q * 8:q * 8 + 8, :]
            return 0
        lax.fori_loop(0, groups, ungroup, 0)
        for b in range(nblk):
            cp = pltpu.make_async_copy(raw.at[f, b, pl.ds(halo, rows), :], dst.at[:, pl.ds(b * 128, 128)],
                                       out_sem.at[f, b])
            cp.start()
            outs.append(cp)
    for cp in outs:
        cp.wait()


def solution(mesh):
    tile_spec = P(("ens", "row"), "col")

    def local_run(u_tile, v_tile, stencil_w):
        rows, cols = u_tile.shape
        steps = stencil_w.shape[0]
        halo = HALO
        R = (rows + 2 * halo) // 8
        nblk = cols // 128
        f32 = jnp.float32
        dma = pltpu.SemaphoreType.DMA
        return pl.pallas_call(
            functools.partial(kernel, steps, rows, cols, halo, CHUNK),
            out_shape=[jax.ShapeDtypeStruct((rows, cols), f32)] * 2,
            in_specs=[pl.BlockSpec(memory_space=pltpu.SMEM)] + [pl.BlockSpec(memory_space=pl.ANY)] * 2,
            out_specs=[pl.BlockSpec(memory_space=pl.ANY)] * 2,
            scratch_shapes=[
                pltpu.VMEM((2, nblk + 1, 8 * R, 128), f32),
                pltpu.VMEM((2, rows, 128), f32),
                pltpu.VMEM((R * NB * 8, 128), f32),
                pltpu.VMEM((R * NB * 8, 128), f32),
                pltpu.VMEM((128 * NC, 128), f32),
                pltpu.VMEM((2, 2, 2, halo // 8, NC, 8, 128), f32),
                pltpu.VMEM((2, 2, 2, halo // 8, NC, 8, 128), f32),
                dma((2, nblk)), dma((2, 2)), dma((2, 2, 2)), dma((2, 2, 2)), dma((2, 2, 2)), dma((2, 2, 2)), dma((2, nblk)),
            ],
            compiler_params=pltpu.CompilerParams(collective_id=0, has_side_effects=True,
                                                 vmem_limit_bytes=48 * 1024 * 1024),
        )(stencil_w, u_tile, v_tile)

    return jax.shard_map(local_run, mesh=mesh, in_specs=(tile_spec, tile_spec, P()), out_specs=(tile_spec, tile_spec), check_vma=False)
```

```python
import functools

import jax
import jax.numpy as jnp
from jax import lax
from jax.experimental import pallas as pl
from jax.experimental.pallas import tpu as pltpu
from jax.sharding import PartitionSpec as P

HALO = 16
PARTS = 2
NC = 9
NB = 11
SCALE = 0.125
MESH = pl.DeviceIdType.MESH


def kernel(steps, rows, cols, halo, w_ref, u_hbm, v_hbm, uo_hbm, vo_hbm,
           raw, gsend, state_a, state_b, coef, wide, sbuf, rbuf,
           load_sem, col_sems, row_sems, diag_sems, send_sems, recv_sems, out_sem):
    R = (rows + 2 * halo) // 8
    nblk = cols // 128
    n_row = lax.axis_size("row")
    me_row, me_col = lax.axis_index("row"), lax.axis_index("col")
    up, down = lax.rem(me_row + n_row - 1, n_row), lax.rem(me_row + 1, n_row)
    other = 1 - me_col

    loads = []
    for f, src in enumerate((u_hbm, v_hbm)):
        for b in (0, nblk - 1, *range(1, nblk - 1)):
            cp = pltpu.make_async_copy(src.at[:, pl.ds(b * 128, 128)],
                                       raw.at[f, b, pl.ds(halo, rows), :], load_sem.at[f, b])
            cp.start()
            loads.append(cp)

    barrier = pltpu.get_barrier_semaphore()
    peers = [(up, me_col), (down, me_col), (me_row, other), (up, other), (down, other)]
    for r, c in peers:
        pl.semaphore_signal(barrier, inc=1, device_id={"row": r, "col": c}, device_id_type=MESH)
    pl.semaphore_wait(barrier, len(peers))

    states = (state_a, state_b)
    lane = lax.broadcasted_iota(jnp.int32, (8, 128), 1)

    def remote(src, dst, sems, r, c):
        cp = pltpu.make_async_remote_copy(src_ref=src, dst_ref=dst, send_sem=sems.at[0], recv_sem=sems.at[1],
                                          device_id={"row": r, "col": c}, device_id_type=MESH)
        cp.start()
        return cp

    halos = []
    for f in range(2):
        mine = loads[f * nblk:(f + 1) * nblk]
        mine[0].wait()
        mine[1].wait()

        def build(i, _, f=f):
            for q in range(8):
                at = pl.multiple_of(i * 64 + q * 8, 8)
                gsend[f, pl.ds(at, 8), :] = jnp.where(lane < 64, raw[f, 0, pl.ds(halo + at, 8), :],
                                                      raw[f, nblk - 1, pl.ds(halo + at, 8), :])
            return 0
        lax.fori_loop(0, rows // 64, build, 0)
        cols_in = [
            remote(gsend.at[f], raw.at[f, nblk, pl.ds(halo, rows), :], col_sems.at[f], me_row, other),
            remote(gsend.at[f, pl.ds(0, halo), :], raw.at[f, nblk, pl.ds(halo + rows, halo), :],
                   diag_sems.at[f, 0], up, other),
            remote(gsend.at[f, pl.ds(rows - halo, halo), :], raw.at[f, nblk, pl.ds(0, halo), :],
                   diag_sems.at[f, 1], down, other)]
        for cp in mine[2:]:
            cp.wait()
        rows_in = [
            remote(raw.at[f, pl.ds(0, nblk), pl.ds(halo, halo), :],
                   raw.at[f, pl.ds(0, nblk), pl.ds(halo + rows, halo), :], row_sems.at[f, 0], up, me_col),
            remote(raw.at[f, pl.ds(0, nblk), pl.ds(rows, halo), :],
                   raw.at[f, pl.ds(0, nblk), pl.ds(0, halo), :], row_sems.at[f, 1], down, me_col)]
        halos.append((rows_in, cols_in))

    w = lambda i, j: w_ref[i, j:j + 1, :]
    for k, row in enumerate((0.25 * (w(0, 0) + w(0, 2)), 0.25 * (w(0, 2) - w(0, 0)), 0.5 * w(0, 1),
                              0.5 * w(1, 0), 1.5 + 0.5 * w(1, 1))):
        coef[k] = jnp.broadcast_to(row, (128, steps)).T

    groups = R // 16
    spare = R % 16

    def reg(r, c):
        return pl.ds(pl.multiple_of((r * NB + c + 1) * 8, 8), 8)

    def line(r, shift=0):
        return pl.ds(pl.multiple_of((r * NB + 1 + shift) * 8, 8), NC * 8)

    def to_lanes(f, i, n, blocks):
        for b in blocks:
            parts = []
            for q in range(n):
                at = pl.ds(i * 16 + q, 8, stride=R)
                x = raw[0, b, at, :]
                if f == 1:
                    x = x - 0.5 * raw[1, b, at, :]
                parts.append(x * SCALE)
            wide[f, i, pl.ds(b * 128, 128), :8 * n] = jnp.concatenate(parts, axis=0).T

    def to_registers(f, i, n):
        for c in range(NC):
            back = wide[f, i, pl.ds(c, 128, stride=NC), :][:, :8 * n].T
            for q in range(n):
                r = i * 16 + q
                x = back[q * 8:q * 8 + 8, :]
                if f == 1:
                    x = state_b[reg(r, c), :] - x
                states[f][reg(r, c), :] = x
                if c == 0:
                    states[f][reg(r, NC), :] = pltpu.roll(x, 127, 1)
                if c == NC - 1:
                    states[f][reg(r, -1), :] = pltpu.roll(x, 1, 1)

    def over_groups(fn):
        lax.fori_loop(0, groups, lambda i, _: (fn(i, 16), 0)[1], 0)
        if spare:
            fn(groups, spare)

    def convert(f):
        for cp in halos[f][0]:
            cp.wait()
        over_groups(lambda i, n: to_lanes(f, i, n, range(nblk)))
        for cp in halos[f][1]:
            cp.wait()
        over_groups(lambda i, n: to_lanes(f, i, n, (nblk,)))
        over_groups(lambda i, n: to_registers(f, i, n))

    def clear(r, _):
        state_b[line(r), :] = jnp.zeros((NC * 8, 128), jnp.float32)
        return 0
    lax.fori_loop(0, R, clear, 0)
    convert(0)

    def level(t, cur, new):
        alpha, beta, side, mid_s, centre = (coef[k, pl.ds(t, 1), :] for k in range(5))

        def contrib(r):
            left, here, right = cur[line(r, -1), :], cur[line(r), :], cur[line(r, 1), :]
            s, d = left + right, right - left
            e, bd = alpha * s + side * here, beta * d
            return e + bd, mid_s * s + centre * here, e - bd

        def edges(ref, r):
            ref[reg(r, NC), :] = pltpu.roll(ref[reg(r, 0), :], 127, 1)
            ref[reg(r, -1), :] = pltpu.roll(ref[reg(r, NC - 1), :], 1, 1)

        def turn(x, by):
            return jnp.concatenate([pltpu.roll(x[8 * c:8 * c + 8, :], by, 0) for c in range(NC)], axis=0)

        half = R // 2
        part = half // PARTS

        def sweep(first, step, seam_turn, lag):
            fwd, back = (0, 2) if step > 0 else (2, 0)
            here = contrib(first)
            away, acc = here[fwd], turn(contrib(R - 1 - first)[fwd], seam_turn) + here[1]
            for it in range(PARTS):
                for q in range(part):
                    lag(it, q)
                for q in range(part):
                    r = first + step * (it * part + q)
                    nxt = contrib(r + step)
                    new[line(r), :] = (acc + nxt[back]) - new[line(r), :]
                    away, acc = nxt[fwd], away + nxt[1]

        def lag_down(it, q):
            if it == 0:
                edges(cur, half + q)
            else:
                edges(new, (it - 1) * part + q)

        def lag_up(it, q):
            if it == 0:
                edges(new, half - part + q)
            else:
                edges(new, R - it * part + q)
        sweep(0, 1, 1, lag_down)
        sweep(R - 1, -1, 7, lag_up)

    def strided(r, c, s):
        return pl.ds((r * NB + c + 1) * 8 + s, 8, stride=NB * 8)

    def copies(f, slot):
        return [pltpu.make_async_remote_copy(
            src_ref=sbuf.at[slot, d, f], dst_ref=rbuf.at[slot, d, f], send_sem=send_sems.at[slot, d, f],
            recv_sem=recv_sems.at[slot, d, f], device_id={"row": peer, "col": me_col}, device_id_type=MESH)
            for d, peer in enumerate((up, down))]

    def send(f, slot):
        for d, (r0, s) in enumerate(((halo, 0), (R - 2 * halo, 7))):
            for g in range(halo // 8):
                for c in range(NC):
                    sbuf[slot, d, f, g, c] = states[f][strided(r0 + 8 * g, c, s), :]
        for cp in copies(f, slot):
            cp.start()

    def receive(f, slot):
        for d, (r0, s) in enumerate(((R - halo, 7), (0, 0))):
            copies(f, slot)[d].wait()
            for g in range(halo // 8):
                for c in range(NC):
                    states[f][strided(r0 + 8 * g, c, s), :] = rbuf[slot, d, f, g, c]

        def fix(i, _):
            for r0 in (0, R - halo):
                for q in range(8):
                    r = r0 + i * 8 + q
                    states[f][reg(r, NC), :] = pltpu.roll(states[f][reg(r, 0), :], 127, 1)
                    states[f][reg(r, -1), :] = pltpu.roll(states[f][reg(r, NC - 1), :], 1, 1)
            return 0
        lax.fori_loop(0, halo // 8, fix, 0)

    def pair(i, _):
        level(2 * i, state_a, state_b)

        @pl.when(i == 0)
        def _():
            convert(1)
        done = lax.rem(2 * i + 2, halo) == 0
        more = 2 * i + 2 < steps
        slot = lax.rem((2 * i + 2) // halo, 2)

        @pl.when(done & more)
        def _():
            send(1, slot)
        level(2 * i + 1, state_b, state_a)

        @pl.when(done & more)
        def _():
            send(0, slot)
            receive(1, slot)
            receive(0, slot)
        return 0
    lax.fori_loop(0, steps // 2, pair, 0)

    out_groups = (R - 1) // 16
    outs = []
    for f, dst in enumerate((uo_hbm, vo_hbm)):
        def ungroup(i, _, f=f):
            r0 = i * (R - 16) // out_groups
            for c in range(NC):
                parts = []
                for q in range(16):
                    x = state_a[reg(r0 + q, c), :]
                    if f == 1:
                        x = (x - state_b[reg(r0 + q, c), :]) * (2.0 / SCALE)
                    else:
                        x = x * (1.0 / SCALE)
                    parts.append(x)
                wide[f, i, pl.ds(c, 128, stride=NC), :] = jnp.concatenate(parts, axis=0).T
            for b in range(nblk):
                back = wide[f, i, pl.ds(b * 128, 128), :].T
                for q in range(16):
                    raw[f, b, pl.ds(r0 + q, 8, stride=R), :] = back[q * 8:q * 8 + 8, :]
            return 0
        lax.fori_loop(0, out_groups + 1, ungroup, 0)
        for b in range(nblk):
            cp = pltpu.make_async_copy(raw.at[f, b, pl.ds(halo, rows), :], dst.at[:, pl.ds(b * 128, 128)],
                                       out_sem.at[f, b])
            cp.start()
            outs.append(cp)
    for cp in outs:
        cp.wait()


def solution(mesh):
    tile_spec = P(("ens", "row"), "col")

    def local_run(u_tile, v_tile, stencil_w):
        rows, cols = u_tile.shape
        steps = stencil_w.shape[0]
        halo = HALO
        R = (rows + 2 * halo) // 8
        nblk = cols // 128
        f32 = jnp.float32
        dma = pltpu.SemaphoreType.DMA
        return pl.pallas_call(
            functools.partial(kernel, steps, rows, cols, halo),
            out_shape=[jax.ShapeDtypeStruct((rows, cols), f32)] * 2,
            in_specs=[pl.BlockSpec(memory_space=pltpu.VMEM)] + [pl.BlockSpec(memory_space=pl.ANY)] * 2,
            out_specs=[pl.BlockSpec(memory_space=pl.ANY)] * 2,
            scratch_shapes=[
                pltpu.VMEM((2, nblk + 1, 8 * R, 128), f32),
                pltpu.VMEM((2, rows, 128), f32),
                pltpu.VMEM((R * NB * 8, 128), f32),
                pltpu.VMEM((R * NB * 8, 128), f32),
                pltpu.VMEM((5, steps, 128), f32),
                pltpu.VMEM((2, -(-R // 16), 128 * NC, 128), f32),
                pltpu.VMEM((2, 2, 2, halo // 8, NC, 8, 128), f32),
                pltpu.VMEM((2, 2, 2, halo // 8, NC, 8, 128), f32),
                dma((2, nblk)), dma((2, 2)), dma((2, 2, 2)), dma((2, 2, 2)), dma((2, 2, 2)), dma((2, 2, 2)), dma((2, nblk)),
            ],
            compiler_params=pltpu.CompilerParams(collective_id=0, has_side_effects=True,
                                                 vmem_limit_bytes=48 * 1024 * 1024),
        )(stencil_w.transpose(1, 2, 0), u_tile, v_tile)

    return jax.shard_map(local_run, mesh=mesh, in_specs=(tile_spec, tile_spec, P()), out_specs=(tile_spec, tile_spec), check_vma=False)
```

```python
import functools

import jax
import jax.numpy as jnp
from jax import lax
from jax.experimental import pallas as pl
from jax.experimental.pallas import tpu as pltpu
from jax.sharding import PartitionSpec as P

HALO = 16
AHEAD = 4
NC = 9
NB = 11
SCALE = 0.125
MESH = pl.DeviceIdType.MESH


def kernel(steps, rows, cols, halo, w_ref, u_hbm, v_hbm, uo_hbm, vo_hbm,
           raw, gsend, state_a, state_b, coef, wide, sbuf, rbuf,
           load_sem, col_sems, row_sems, diag_sems, send_sems, recv_sems, out_sem):
    R = (rows + 2 * halo) // 8
    nblk = cols // 128
    n_row = lax.axis_size("row")
    me_row, me_col = lax.axis_index("row"), lax.axis_index("col")
    up, down = lax.rem(me_row + n_row - 1, n_row), lax.rem(me_row + 1, n_row)
    other = 1 - me_col

    loads = []
    for f, src in enumerate((u_hbm, v_hbm)):
        for b in (0, nblk - 1, *range(1, nblk - 1)):
            cp = pltpu.make_async_copy(src.at[:, pl.ds(b * 128, 128)],
                                       raw.at[f, b, pl.ds(halo, rows), :], load_sem.at[f, b])
            cp.start()
            loads.append(cp)

    barrier = pltpu.get_barrier_semaphore()
    peers = [(up, me_col), (down, me_col), (me_row, other), (up, other), (down, other)]
    for r, c in peers:
        pl.semaphore_signal(barrier, inc=1, device_id={"row": r, "col": c}, device_id_type=MESH)
    pl.semaphore_wait(barrier, len(peers))

    states = (state_a, state_b)
    lane = lax.broadcasted_iota(jnp.int32, (8, 128), 1)

    def remote(src, dst, sems, r, c):
        cp = pltpu.make_async_remote_copy(src_ref=src, dst_ref=dst, send_sem=sems.at[0], recv_sem=sems.at[1],
                                          device_id={"row": r, "col": c}, device_id_type=MESH)
        cp.start()
        return cp

    halos = []
    for f in range(2):
        mine = loads[f * nblk:(f + 1) * nblk]
        mine[0].wait()
        mine[1].wait()

        def build(i, _, f=f):
            for q in range(8):
                at = pl.multiple_of(i * 64 + q * 8, 8)
                gsend[f, pl.ds(at, 8), :] = jnp.where(lane < 64, raw[f, 0, pl.ds(halo + at, 8), :],
                                                      raw[f, nblk - 1, pl.ds(halo + at, 8), :])
            return 0
        lax.fori_loop(0, rows // 64, build, 0)
        cols_in = [
            remote(gsend.at[f], raw.at[f, nblk, pl.ds(halo, rows), :], col_sems.at[f], me_row, other),
            remote(gsend.at[f, pl.ds(0, halo), :], raw.at[f, nblk, pl.ds(halo + rows, halo), :],
                   diag_sems.at[f, 0], up, other),
            remote(gsend.at[f, pl.ds(rows - halo, halo), :], raw.at[f, nblk, pl.ds(0, halo), :],
                   diag_sems.at[f, 1], down, other)]
        for cp in mine[2:]:
            cp.wait()
        rows_in = [
            remote(raw.at[f, pl.ds(0, nblk), pl.ds(halo, halo), :],
                   raw.at[f, pl.ds(0, nblk), pl.ds(halo + rows, halo), :], row_sems.at[f, 0], up, me_col),
            remote(raw.at[f, pl.ds(0, nblk), pl.ds(rows, halo), :],
                   raw.at[f, pl.ds(0, nblk), pl.ds(0, halo), :], row_sems.at[f, 1], down, me_col)]
        halos.append((rows_in, cols_in))

    w = lambda i, j: w_ref[i, j:j + 1, :]
    for k, row in enumerate((0.25 * (w(0, 0) + w(0, 2)), 0.25 * (w(0, 2) - w(0, 0)), 0.5 * w(0, 1),
                              0.5 * w(1, 0), 1.5 + 0.5 * w(1, 1))):
        coef[k] = jnp.broadcast_to(row, (128, steps)).T

    groups = R // 16
    spare = R % 16

    def reg(r, c):
        return pl.ds(pl.multiple_of((r * NB + c + 1) * 8, 8), 8)

    def line(r, shift=0):
        return pl.ds(pl.multiple_of((r * NB + 1 + shift) * 8, 8), NC * 8)

    def in_registers(base, q, c):
        return pl.ds(pl.multiple_of(base + (q * NB + c + 1) * 8, 8), 8)

    def to_lanes(f, i, n, blocks):
        r0 = i * 16
        for b in blocks:
            x = jnp.concatenate([raw[f, b, pl.ds(r0 + q, 8, stride=R), :] for q in range(n)], axis=0)
            wide[f, i, pl.ds(b * 128, 128), :8 * n] = (x * (0.5 * SCALE if f else SCALE)).T

    def to_registers(f, i, n):
        base = i * (16 * NB * 8)
        for c in range(NC):
            back = wide[f, i, pl.ds(c, 128, stride=NC), :][:, :8 * n].T
            if f == 1:
                back = jnp.concatenate([state_b[in_registers(base, q, c), :] for q in range(n)], axis=0) + back
            puts = [(c, back)]
            if c == 0:
                puts.append((NC, pltpu.roll(back, 127, 1)))
            if c == NC - 1:
                puts.append((-1, pltpu.roll(back, 1, 1)))
            for to, x in puts:
                for q in range(n):
                    states[f][in_registers(base, q, to), :] = x[q * 8:q * 8 + 8, :]

    def over_groups(fn):
        lax.fori_loop(0, groups, lambda i, _: (fn(i, 16), 0)[1], 0)
        if spare:
            fn(groups, spare)

    def convert(f):
        for cp in halos[f][0]:
            cp.wait()
        over_groups(lambda i, n: to_lanes(f, i, n, range(nblk)))
        for cp in halos[f][1]:
            cp.wait()
        over_groups(lambda i, n: to_lanes(f, i, n, (nblk,)))
        over_groups(lambda i, n: to_registers(f, i, n))

    convert(0)

    def same(r, _):
        state_b[line(r), :] = state_a[line(r), :]
        return 0
    lax.fori_loop(0, R, same, 0)

    def step(t, cur, new):
        alpha, beta, side, mid_s, centre = (
            jnp.broadcast_to(coef[k, pl.ds(t, 1), :], (NC * 8, 128)) for k in range(5))

        def contrib(r):
            left, here, right = cur[line(r, -1), :], cur[line(r), :], cur[line(r, 1), :]
            s, d = left + right, right - left
            e, bd = alpha * s + side * here, beta * d
            return e + bd, mid_s * s + centre * here, e - bd

        def store(r, x):
            new[line(r), :] = x - new[line(r), :]
        return contrib, store, new

    def edges(ref, r):
        at = lambda c: pl.ds((r * NB + c + 1) * 8, 8)
        ref[at(NC), :] = pltpu.roll(ref[at(0), :], 127, 1)
        ref[at(-1), :] = pltpu.roll(ref[at(NC - 1), :], 1, 1)

    def turn(x, by):
        return jnp.concatenate([pltpu.roll(x[8 * c:8 * c + 8, :], by, 0) for c in range(NC)], axis=0)

    def cross(x, r, to):
        if (r, to) == (R - 1, 0):
            return turn(x, 1)
        return turn(x, 7) if (r, to) == (0, R - 1) else x

    def arc(at, first, count, way, late):
        contrib, store, new = at
        fwd, back = (0, 2) if way > 0 else (2, 0)
        before, r = (first - way) % R, first % R
        here = contrib(r)
        away, acc = here[fwd], cross(contrib(before)[fwd], before, r) + here[1]
        for n in (count // 2, count - count // 2):
            for ref, row in late:
                edges(ref, row)
            late = []
            for _ in range(n):
                to = (r + way) % R
                nxt = contrib(to)
                store(r, acc + cross(nxt[back], to, r))
                away, acc = nxt[fwd], cross(away, r, to) + nxt[1]
                late.append((new, r))
                r = to
        return late

    half = R // 2

    def level(t, cur, new):
        at = step(t, cur, new)
        late = arc(at, 0, half, 1, [(cur, half + q) for q in range(half - half // 2)])
        arc(at, R - 1, R - half, -1, late)

    def strided(r, c, s):
        return pl.ds((r * NB + c + 1) * 8 + s, 8, stride=NB * 8)

    def copies(f, slot):
        return [pltpu.make_async_remote_copy(
            src_ref=sbuf.at[slot, d, f], dst_ref=rbuf.at[slot, d, f], send_sem=send_sems.at[slot, d, f],
            recv_sem=recv_sems.at[slot, d, f], device_id={"row": peer, "col": me_col}, device_id_type=MESH)
            for d, peer in enumerate((up, down))]

    def send(f, slot):
        for d, (r0, s) in enumerate(((halo, 0), (R - 2 * halo, 7))):
            for g in range(halo // 8):
                for c in range(NC):
                    sbuf[slot, d, f, g, c] = states[f][strided(r0 + 8 * g, c, s), :]
        for cp in copies(f, slot):
            cp.start()

    def receive(f, slot):
        for d, (r0, s) in enumerate(((R - halo, 7), (0, 0))):
            copies(f, slot)[d].wait()
            for g in range(halo // 8):
                for c in range(NC):
                    states[f][strided(r0 + 8 * g, c, s), :] = rbuf[slot, d, f, g, c]

    def after_exchange(t0, slot):
        at = [step(t0 + j, states[j % 2], states[1 - j % 2]) for j in range(AHEAD)]
        late = [(state_a, half + q) for q in range(half - half // 2)]
        for j in range(AHEAD):
            late = arc(at[j], halo + 1 + j, R - 2 * halo - 2 - 2 * j, 1, late)
        receive(1, slot)
        receive(0, slot)
        for r in (*range(halo), *range(R - halo, R)):
            edges(state_a, r)
        for j in range(AHEAD):
            late = arc(at[j], R - halo - 1 - j, 2 * halo + 2 + 2 * j, 1, late)
        for ref, r in late:
            edges(ref, r)

    def pair(i, _):
        level(2 * i, state_a, state_b)
        nth = (i + 1) * 2 // halo
        leave = (lax.rem(2 * i + 2, halo) == 0) & (2 * i + 2 < steps)

        @pl.when(i == 0)
        def _():
            convert(1)

        @pl.when(leave)
        def _():
            send(1, lax.rem(nth, 2))
        level(2 * i + 1, state_b, state_a)

        @pl.when(leave)
        def _():
            send(0, lax.rem(nth, 2))
        return 0

    phases = steps // halo

    def phase(p, _):
        @pl.when(p > 0)
        def _():
            after_exchange(p * halo, lax.rem(p, 2))
        lax.fori_loop(p * (halo // 2) + (p + phases - 1) // phases * (AHEAD // 2), (p + 1) * (halo // 2), pair, 0)
        return 0
    lax.fori_loop(0, phases, phase, 0)

    out_groups = (R - 1) // 16
    outs = []
    for f, dst in enumerate((uo_hbm, vo_hbm)):
        def ungroup(i, _, f=f):
            r0 = i * (R - 16) // out_groups
            base = r0 * (NB * 8)

            def gathered(ref, c):
                return jnp.concatenate([ref[in_registers(base, q, c), :] for q in range(16)], axis=0)
            for c in range(NC):
                x = gathered(state_a, c)
                x = x * (1.0 / SCALE) if f == 0 else (x - gathered(state_b, c)) * (2.0 / SCALE)
                wide[f, i, pl.ds(c, 128, stride=NC), :] = x.T
            for b in range(nblk):
                back = wide[f, i, pl.ds(b * 128, 128), :].T
                for q in range(16):
                    raw[f, b, pl.ds(r0 + q, 8, stride=R), :] = back[q * 8:q * 8 + 8, :]
            return 0
        lax.fori_loop(0, out_groups + 1, ungroup, 0)
        for b in range(nblk):
            cp = pltpu.make_async_copy(raw.at[f, b, pl.ds(halo, rows), :], dst.at[:, pl.ds(b * 128, 128)],
                                       out_sem.at[f, b])
            cp.start()
            outs.append(cp)
    for cp in outs:
        cp.wait()


def solution(mesh):
    tile_spec = P(("ens", "row"), "col")

    def local_run(u_tile, v_tile, stencil_w):
        rows, cols = u_tile.shape
        steps = stencil_w.shape[0]
        halo = HALO
        R = (rows + 2 * halo) // 8
        nblk = cols // 128
        f32 = jnp.float32
        dma = pltpu.SemaphoreType.DMA
        return pl.pallas_call(
            functools.partial(kernel, steps, rows, cols, halo),
            out_shape=[jax.ShapeDtypeStruct((rows, cols), f32)] * 2,
            in_specs=[pl.BlockSpec(memory_space=pltpu.VMEM)] + [pl.BlockSpec(memory_space=pl.ANY)] * 2,
            out_specs=[pl.BlockSpec(memory_space=pl.ANY)] * 2,
            scratch_shapes=[
                pltpu.VMEM((2, nblk + 1, 8 * R, 128), f32),
                pltpu.VMEM((2, rows, 128), f32),
                pltpu.VMEM((R * NB * 8, 128), f32),
                pltpu.VMEM((R * NB * 8, 128), f32),
                pltpu.VMEM((5, steps, 128), f32),
                pltpu.VMEM((2, -(-R // 16), 128 * NC, 128), f32),
                pltpu.VMEM((2, 2, 2, halo // 8, NC, 8, 128), f32),
                pltpu.VMEM((2, 2, 2, halo // 8, NC, 8, 128), f32),
                dma((2, nblk)), dma((2, 2)), dma((2, 2, 2)), dma((2, 2, 2)), dma((2, 2, 2)), dma((2, 2, 2)), dma((2, nblk)),
            ],
            compiler_params=pltpu.CompilerParams(collective_id=0, has_side_effects=True,
                                                 vmem_limit_bytes=48 * 1024 * 1024),
        )(stencil_w.transpose(1, 2, 0), u_tile, v_tile)

    return jax.shard_map(local_run, mesh=mesh, in_specs=(tile_spec, tile_spec, P()), out_specs=(tile_spec, tile_spec), check_vma=False)
```

```python
import functools

import jax
import jax.numpy as jnp
from jax import lax
from jax.experimental import pallas as pl
from jax.experimental.pallas import tpu as pltpu
from jax.sharding import PartitionSpec as P

HALO = 16
AHEAD = 4
NC = 9
NB = 11
SCALE = 0.125
MESH = pl.DeviceIdType.MESH


def kernel(steps, rows, cols, halo, w_hbm, u_hbm, v_hbm, state_a, state_b,
           raw, gsend, w_ref, coef, wide, sbuf, rbuf,
           load_sem, col_sems, row_sems, diag_sems, send_sems, recv_sems, w_sem):
    R = (rows + 2 * halo) // 8
    nblk = cols // 128
    n_row = lax.axis_size("row")
    me_row, me_col = lax.axis_index("row"), lax.axis_index("col")
    up, down = lax.rem(me_row + n_row - 1, n_row), lax.rem(me_row + 1, n_row)
    other = 1 - me_col

    weights = pltpu.make_async_copy(w_hbm, w_ref, w_sem)
    weights.start()

    loads = []
    for f, src in enumerate((u_hbm, v_hbm)):
        for b in (0, nblk - 1, *range(1, nblk - 1)):
            cp = pltpu.make_async_copy(src.at[:, pl.ds(b * 128, 128)],
                                       raw.at[f, b, pl.ds(halo, rows), :], load_sem.at[f, b])
            cp.start()
            loads.append(cp)

    barrier = pltpu.get_barrier_semaphore()
    peers = [(up, me_col), (down, me_col), (me_row, other), (up, other), (down, other)]
    for r, c in peers:
        pl.semaphore_signal(barrier, inc=1, device_id={"row": r, "col": c}, device_id_type=MESH)
    pl.semaphore_wait(barrier, len(peers))

    states = (state_a, state_b)
    lane = lax.broadcasted_iota(jnp.int32, (8, 128), 1)

    def remote(src, dst, sems, r, c):
        cp = pltpu.make_async_remote_copy(src_ref=src, dst_ref=dst, send_sem=sems.at[0], recv_sem=sems.at[1],
                                          device_id={"row": r, "col": c}, device_id_type=MESH)
        cp.start()
        return cp

    halos = []
    for f in range(2):
        mine = loads[f * nblk:(f + 1) * nblk]
        mine[0].wait()
        mine[1].wait()

        def build(i, _, f=f):
            for q in range(8):
                at = pl.multiple_of(i * 64 + q * 8, 8)
                gsend[f, pl.ds(at, 8), :] = jnp.where(lane < 64, raw[f, 0, pl.ds(halo + at, 8), :],
                                                      raw[f, nblk - 1, pl.ds(halo + at, 8), :])
            return 0
        lax.fori_loop(0, rows // 64, build, 0)
        cols_in = [
            remote(gsend.at[f], raw.at[f, nblk, pl.ds(halo, rows), :], col_sems.at[f], me_row, other),
            remote(gsend.at[f, pl.ds(0, halo), :], raw.at[f, nblk, pl.ds(halo + rows, halo), :],
                   diag_sems.at[f, 0], up, other),
            remote(gsend.at[f, pl.ds(rows - halo, halo), :], raw.at[f, nblk, pl.ds(0, halo), :],
                   diag_sems.at[f, 1], down, other)]
        for cp in mine[2:]:
            cp.wait()
        rows_in = [
            remote(raw.at[f, pl.ds(0, nblk), pl.ds(halo, halo), :],
                   raw.at[f, pl.ds(0, nblk), pl.ds(halo + rows, halo), :], row_sems.at[f, 0], up, me_col),
            remote(raw.at[f, pl.ds(0, nblk), pl.ds(rows, halo), :],
                   raw.at[f, pl.ds(0, nblk), pl.ds(0, halo), :], row_sems.at[f, 1], down, me_col)]
        halos.append((rows_in, cols_in))

    weights.wait()
    w = lambda i, j: w_ref[i, j:j + 1, :]
    for k, row in enumerate((0.25 * (w(0, 0) + w(0, 2)), 0.25 * (w(0, 2) - w(0, 0)), 0.5 * w(0, 1),
                              0.5 * w(1, 0), 1.5 + 0.5 * w(1, 1))):
        coef[k] = jnp.broadcast_to(row, (128, steps)).T

    groups = R // 16
    spare = R % 16

    def reg(r, c):
        return pl.ds(pl.multiple_of((r * NB + c + 1) * 8, 8), 8)

    def line(r, shift=0):
        return pl.ds(pl.multiple_of((r * NB + 1 + shift) * 8, 8), NC * 8)

    def in_registers(base, q, c):
        return pl.ds(pl.multiple_of(base + (q * NB + c + 1) * 8, 8), 8)

    def to_lanes(f, i, n, blocks):
        r0 = i * 16
        for b in blocks:
            x = jnp.concatenate([raw[f, b, pl.ds(r0 + q, 8, stride=R), :] for q in range(n)], axis=0)
            wide[f, i, pl.ds(b * 128, 128), :8 * n] = (x * (0.5 * SCALE if f else SCALE)).T

    def to_registers(f, i, n):
        base = i * (16 * NB * 8)
        for c in range(NC):
            back = wide[f, i, pl.ds(c, 128, stride=NC), :][:, :8 * n].T
            if f == 1:
                back = jnp.concatenate([state_b[in_registers(base, q, c), :] for q in range(n)], axis=0) + back
            puts = [(c, back)]
            if c == 0:
                puts.append((NC, pltpu.roll(back, 127, 1)))
            if c == NC - 1:
                puts.append((-1, pltpu.roll(back, 1, 1)))
            for to, x in puts:
                for q in range(n):
                    states[f][in_registers(base, q, to), :] = x[q * 8:q * 8 + 8, :]

    def over_groups(fn):
        lax.fori_loop(0, groups, lambda i, _: (fn(i, 16), 0)[1], 0)
        if spare:
            fn(groups, spare)

    def convert(f):
        for cp in halos[f][0]:
            cp.wait()
        over_groups(lambda i, n: to_lanes(f, i, n, range(nblk)))
        for cp in halos[f][1]:
            cp.wait()
        over_groups(lambda i, n: to_lanes(f, i, n, (nblk,)))
        over_groups(lambda i, n: to_registers(f, i, n))

    convert(0)

    def same(r, _):
        state_b[line(r), :] = state_a[line(r), :]
        return 0
    lax.fori_loop(0, R, same, 0)

    def step(t, cur, new):
        alpha, beta, side, mid_s, centre = (
            jnp.broadcast_to(coef[k, pl.ds(t, 1), :], (NC * 8, 128)) for k in range(5))

        def contrib(r):
            left, here, right = cur[line(r, -1), :], cur[line(r), :], cur[line(r, 1), :]
            s, d = left + right, right - left
            e, bd = alpha * s + side * here, beta * d
            return e + bd, mid_s * s + centre * here, e - bd

        def store(r, x):
            new[line(r), :] = x - new[line(r), :]
        return contrib, store, new

    def edges(ref, r):
        at = lambda c: pl.ds((r * NB + c + 1) * 8, 8)
        ref[at(NC), :] = pltpu.roll(ref[at(0), :], 127, 1)
        ref[at(-1), :] = pltpu.roll(ref[at(NC - 1), :], 1, 1)

    def turn(x, by):
        return jnp.concatenate([pltpu.roll(x[8 * c:8 * c + 8, :], by, 0) for c in range(NC)], axis=0)

    def cross(x, r, to):
        if (r, to) == (R - 1, 0):
            return turn(x, 1)
        return turn(x, 7) if (r, to) == (0, R - 1) else x

    def arc(at, first, count, way, late):
        contrib, store, new = at
        fwd, back = (0, 2) if way > 0 else (2, 0)
        before, r = (first - way) % R, first % R
        here = contrib(r)
        away, acc = here[fwd], cross(contrib(before)[fwd], before, r) + here[1]
        for n in (count // 2, count - count // 2):
            for ref, row in late:
                edges(ref, row)
            late = []
            for _ in range(n):
                to = (r + way) % R
                nxt = contrib(to)
                store(r, acc + cross(nxt[back], to, r))
                away, acc = nxt[fwd], cross(away, r, to) + nxt[1]
                late.append((new, r))
                r = to
        return late

    half = R // 2

    def level(t, cur, new):
        at = step(t, cur, new)
        late = arc(at, 0, half, 1, [(cur, half + q) for q in range(half - half // 2)])
        arc(at, R - 1, R - half, -1, late)

    def strided(r, c, s):
        return pl.ds((r * NB + c + 1) * 8 + s, 8, stride=NB * 8)

    def copies(f, slot):
        return [pltpu.make_async_remote_copy(
            src_ref=sbuf.at[slot, d, f], dst_ref=rbuf.at[slot, d, f], send_sem=send_sems.at[slot, d, f],
            recv_sem=recv_sems.at[slot, d, f], device_id={"row": peer, "col": me_col}, device_id_type=MESH)
            for d, peer in enumerate((up, down))]

    def send(f, slot):
        for d, (r0, s) in enumerate(((halo, 0), (R - 2 * halo, 7))):
            for g in range(halo // 8):
                for c in range(NC):
                    sbuf[slot, d, f, g, c] = states[f][strided(r0 + 8 * g, c, s), :]
        for cp in copies(f, slot):
            cp.start()

    def receive(f, slot):
        for d, (r0, s) in enumerate(((R - halo, 7), (0, 0))):
            copies(f, slot)[d].wait()
            for g in range(halo // 8):
                for c in range(NC):
                    states[f][strided(r0 + 8 * g, c, s), :] = rbuf[slot, d, f, g, c]

    def after_exchange(t0, slot):
        at = [step(t0 + j, states[j % 2], states[1 - j % 2]) for j in range(AHEAD)]
        late = [(state_a, half + q) for q in range(half - half // 2)]
        for j in range(AHEAD):
            late = arc(at[j], halo + 1 + j, R - 2 * halo - 2 - 2 * j, 1, late)
        receive(1, slot)
        receive(0, slot)
        for r in (*range(halo), *range(R - halo, R)):
            edges(state_a, r)
        for j in range(AHEAD):
            late = arc(at[j], R - halo - 1 - j, 2 * halo + 2 + 2 * j, 1, late)
        for ref, r in late:
            edges(ref, r)

    def pair(i, _):
        level(2 * i, state_a, state_b)
        nth = (i + 1) * 2 // halo
        leave = (lax.rem(2 * i + 2, halo) == 0) & (2 * i + 2 < steps)

        @pl.when(i == 0)
        def _():
            convert(1)

        @pl.when(leave)
        def _():
            send(1, lax.rem(nth, 2))
        level(2 * i + 1, state_b, state_a)

        @pl.when(leave)
        def _():
            send(0, lax.rem(nth, 2))
        return 0

    phases = steps // halo

    def phase(p, _):
        @pl.when(p > 0)
        def _():
            after_exchange(p * halo, lax.rem(p, 2))
        lax.fori_loop(p * (halo // 2) + (p + phases - 1) // phases * (AHEAD // 2), (p + 1) * (halo // 2), pair, 0)
        return 0
    lax.fori_loop(0, phases, phase, 0)


def unpack_kernel(halo, a_ref, b_ref, u_hbm, v_hbm, raw, wide, sems):
    rows, cols = u_hbm.shape
    R = (rows + 2 * halo) // 8
    groups = [(r0, min(16, R - r0)) for r0 in range(0, R, 16)]
    copies = []
    for f, dst in enumerate((u_hbm, v_hbm)):
        for g, (r0, n) in enumerate(groups):
            for c in range(NC):
                parts = []
                for q in range(n):
                    at = pl.ds(((r0 + q) * NB + c + 1) * 8, 8)
                    if f == 0:
                        x = a_ref[at, :] * (1.0 / SCALE)
                    else:
                        x = (a_ref[at, :] - b_ref[at, :]) * (2.0 / SCALE)
                    parts.append(x)
                wide[f, g, pl.ds(c, 128, stride=NC), :8 * n] = jnp.concatenate(parts, axis=0).T
        for b in range(cols // 128):
            for g, (r0, n) in enumerate(groups):
                back = wide[f, g, pl.ds(b * 128, 128), :][:, :8 * n].T
                for q in range(n):
                    raw[f, b, pl.ds(r0 + q, 8, stride=R), :] = back[q * 8:q * 8 + 8, :]
            copies.append(pltpu.make_async_copy(raw.at[f, b, pl.ds(halo, rows), :], dst.at[:, pl.ds(b * 128, 128)],
                                                sems.at[f, b]))
            if len(copies) > 1:
                copies[-2].start()
    copies[-1].start()
    for cp in copies:
        cp.wait()


def solution(mesh):
    tile_spec = P(("ens", "row"), "col")

    def local_run(u_tile, v_tile, stencil_w):
        rows, cols = u_tile.shape
        steps = stencil_w.shape[0]
        halo = HALO
        R = (rows + 2 * halo) // 8
        nblk = cols // 128
        f32 = jnp.float32
        dma = pltpu.SemaphoreType.DMA
        raw = pltpu.VMEM((2, nblk + 1, 8 * R, 128), f32)
        wide = pltpu.VMEM((2, -(-R // 16), 128 * NC, 128), f32)
        vmem, hbm = pl.BlockSpec(memory_space=pltpu.VMEM), pl.BlockSpec(memory_space=pl.ANY)
        states = pl.pallas_call(
            functools.partial(kernel, steps, rows, cols, halo),
            out_shape=[jax.ShapeDtypeStruct((R * NB * 8, 128), f32)] * 2,
            in_specs=[hbm, hbm, hbm],
            out_specs=[vmem, vmem],
            scratch_shapes=[
                raw, pltpu.VMEM((2, rows, 128), f32), pltpu.VMEM((3, 3, steps), f32), pltpu.VMEM((5, steps, 128), f32), wide,
                pltpu.VMEM((2, 2, 2, halo // 8, NC, 8, 128), f32), pltpu.VMEM((2, 2, 2, halo // 8, NC, 8, 128), f32),
                dma((2, nblk)), dma((2, 2)), dma((2, 2, 2)), dma((2, 2, 2)), dma((2, 2, 2)), dma((2, 2, 2)), dma,
            ],
            compiler_params=pltpu.CompilerParams(collective_id=0, has_side_effects=True,
                                                 vmem_limit_bytes=44 * 1024 * 1024),
        )(*(pltpu.with_memory_space_constraint(x, pltpu.HBM) for x in (stencil_w.transpose(1, 2, 0), u_tile, v_tile)))
        return pl.pallas_call(
            functools.partial(unpack_kernel, halo),
            out_shape=[jax.ShapeDtypeStruct((rows, cols), f32)] * 2,
            in_specs=[vmem, vmem],
            out_specs=[hbm, hbm],
            scratch_shapes=[raw, wide, dma((2, nblk))],
            compiler_params=pltpu.CompilerParams(vmem_limit_bytes=32 * 1024 * 1024),
        )(*states)

    return jax.shard_map(local_run, mesh=mesh, in_specs=(tile_spec, tile_spec, P()), out_specs=(tile_spec, tile_spec), check_vma=False)
```

```python
import functools

import jax
import jax.numpy as jnp
from jax import lax
from jax.experimental import pallas as pl
from jax.experimental.pallas import tpu as pltpu
from jax.sharding import PartitionSpec as P

HALO = 16
AHEAD = 6
NC = 9
NB = 11
SCALE = 0.125
MESH = pl.DeviceIdType.MESH


def kernel(steps, rows, cols, halo, w_hbm, u_hbm, v_hbm, state_a, state_b,
           raw, gsend, w_ref, coef, wide, sbuf, rbuf,
           load_sem, col_sems, row_sems, diag_sems, send_sems, recv_sems, w_sem):
    R = (rows + 2 * halo) // 8
    nblk = cols // 128
    n_row = lax.axis_size("row")
    me_row, me_col = lax.axis_index("row"), lax.axis_index("col")
    up, down = lax.rem(me_row + n_row - 1, n_row), lax.rem(me_row + 1, n_row)
    other = 1 - me_col

    weights = pltpu.make_async_copy(w_hbm, w_ref, w_sem)
    weights.start()

    loads = []
    for f, src in enumerate((u_hbm, v_hbm)):
        for b in (0, nblk - 1, *range(1, nblk - 1)):
            cp = pltpu.make_async_copy(src.at[:, pl.ds(b * 128, 128)],
                                       raw.at[f, b, pl.ds(halo, rows), :], load_sem.at[f, b])
            cp.start()
            loads.append(cp)

    barrier = pltpu.get_barrier_semaphore()
    peers = [(up, me_col), (down, me_col), (me_row, other), (up, other), (down, other)]
    for r, c in peers:
        pl.semaphore_signal(barrier, inc=1, device_id={"row": r, "col": c}, device_id_type=MESH)
    pl.semaphore_wait(barrier, len(peers))

    states = (state_a, state_b)
    lane = lax.broadcasted_iota(jnp.int32, (64, 128), 1)

    def remote(src, dst, sems, r, c):
        cp = pltpu.make_async_remote_copy(src_ref=src, dst_ref=dst, send_sem=sems.at[0], recv_sem=sems.at[1],
                                          device_id={"row": r, "col": c}, device_id_type=MESH)
        cp.start()
        return cp

    halos = []
    for f in range(2):
        mine = loads[f * nblk:(f + 1) * nblk]
        mine[0].wait()
        mine[1].wait()

        def build(i, _, f=f):
            at = pl.multiple_of(i * 64, 64)
            gsend[f, pl.ds(at, 64), :] = jnp.where(lane < 64, raw[f, 0, pl.ds(halo + at, 64), :],
                                                   raw[f, nblk - 1, pl.ds(halo + at, 64), :])
            return 0
        lax.fori_loop(0, rows // 64, build, 0)
        cols_in = [
            remote(gsend.at[f], raw.at[f, nblk, pl.ds(halo, rows), :], col_sems.at[f], me_row, other),
            remote(gsend.at[f, pl.ds(0, halo), :], raw.at[f, nblk, pl.ds(halo + rows, halo), :],
                   diag_sems.at[f, 0], up, other),
            remote(gsend.at[f, pl.ds(rows - halo, halo), :], raw.at[f, nblk, pl.ds(0, halo), :],
                   diag_sems.at[f, 1], down, other)]
        for cp in mine[2:]:
            cp.wait()
        rows_in = [
            remote(raw.at[f, pl.ds(0, nblk), pl.ds(halo, halo), :],
                   raw.at[f, pl.ds(0, nblk), pl.ds(halo + rows, halo), :], row_sems.at[f, 0], up, me_col),
            remote(raw.at[f, pl.ds(0, nblk), pl.ds(rows, halo), :],
                   raw.at[f, pl.ds(0, nblk), pl.ds(0, halo), :], row_sems.at[f, 1], down, me_col)]
        halos.append((rows_in, cols_in))

    weights.wait()
    w = lambda i, j: w_ref[i, j:j + 1, :]
    for k, row in enumerate((0.25 * (w(0, 0) + w(0, 2)), 0.25 * (w(0, 2) - w(0, 0)), 0.5 * w(0, 1),
                              0.5 * w(1, 0), 1.5 + 0.5 * w(1, 1))):
        coef[k] = jnp.broadcast_to(row, (128, steps)).T

    groups = R // 16
    spare = R % 16

    def reg(r, c):
        return pl.ds(pl.multiple_of((r * NB + c + 1) * 8, 8), 8)

    def line(r, shift=0):
        return pl.ds(pl.multiple_of((r * NB + 1 + shift) * 8, 8), NC * 8)

    def in_registers(base, q, c):
        return pl.ds(pl.multiple_of(base + (q * NB + c + 1) * 8, 8), 8)

    def to_lanes(f, i, n, blocks):
        r0 = i * 16
        for b in blocks:
            x = jnp.concatenate([raw[f, b, pl.ds(r0 + q, 8, stride=R), :] for q in range(n)], axis=0)
            wide[f, i, pl.ds(b * 128, 128), :8 * n] = (x * (0.5 * SCALE if f else SCALE)).T

    def to_registers(f, i, n):
        base = i * (16 * NB * 8)
        for c in range(NC):
            back = wide[f, i, pl.ds(c, 128, stride=NC), :][:, :8 * n].T
            if f == 1:
                back = jnp.concatenate([state_b[in_registers(base, q, c), :] for q in range(n)], axis=0) + back
            puts = [(c, back)]
            if c == 0:
                puts.append((NC, pltpu.roll(back, 127, 1)))
            if c == NC - 1:
                puts.append((-1, pltpu.roll(back, 1, 1)))
            for to, x in puts:
                for q in range(n):
                    states[f][in_registers(base, q, to), :] = x[q * 8:q * 8 + 8, :]

    def over_groups(fn):
        lax.fori_loop(0, groups, lambda i, _: (fn(i, 16), 0)[1], 0)
        if spare:
            fn(groups, spare)

    def convert(f):
        for cp in halos[f][0]:
            cp.wait()
        over_groups(lambda i, n: to_lanes(f, i, n, range(nblk)))
        for cp in halos[f][1]:
            cp.wait()
        over_groups(lambda i, n: to_lanes(f, i, n, (nblk,)))
        over_groups(lambda i, n: to_registers(f, i, n))

    convert(0)

    def same(r, _):
        state_b[line(r), :] = state_a[line(r), :]
        return 0
    lax.fori_loop(0, R, same, 0)

    def step(t, cur, new):
        alpha, beta, side, mid_s, centre = (
            jnp.broadcast_to(coef[k, pl.ds(t, 1), :], (NC * 8, 128)) for k in range(5))

        def contrib(r):
            left, here, right = cur[line(r, -1), :], cur[line(r), :], cur[line(r, 1), :]
            s, d = left + right, right - left
            e, bd = alpha * s + side * here, beta * d
            return e + bd, mid_s * s + centre * here, e - bd

        def store(r, x):
            at = line(r)
            new[at, :] = x - new[at, :]
        return contrib, store, new

    def edges(ref, r):
        at = lambda c: pl.ds((r * NB + c + 1) * 8, 8)
        ref[at(NC), :] = pltpu.roll(ref[at(0), :], 127, 1)
        ref[at(-1), :] = pltpu.roll(ref[at(NC - 1), :], 1, 1)

    def turn(x, by):
        return jnp.concatenate([pltpu.roll(x[8 * c:8 * c + 8, :], by, 0) for c in range(NC)], axis=0)

    def cross(x, r, to):
        if (r, to) == (R - 1, 0):
            return turn(x, 1)
        return turn(x, 7) if (r, to) == (0, R - 1) else x

    def arc(at, first, count, way, late):
        contrib, store, new = at
        fwd, back = (0, 2) if way > 0 else (2, 0)
        before, r = (first - way) % R, first % R
        here = contrib(r)
        away, acc = here[fwd], cross(contrib(before)[fwd], before, r) + here[1]
        for n in (count // 2, count - count // 2):
            for ref, row in late:
                edges(ref, row)
            late = []
            for _ in range(n):
                to = (r + way) % R
                nxt = contrib(to)
                store(r, acc + cross(nxt[back], to, r))
                away, acc = nxt[fwd], cross(away, r, to) + nxt[1]
                late.append((new, r))
                r = to
        return late

    half = R // 2

    def level(t, cur, new):
        at = step(t, cur, new)
        late = arc(at, 0, half, 1, [(cur, half + q) for q in range(half - half // 2)])
        arc(at, R - 1, R - half, -1, late)

    def strided(r, c, s):
        return pl.ds((r * NB + c + 1) * 8 + s, 8, stride=NB * 8)

    def copies(f, slot):
        return [pltpu.make_async_remote_copy(
            src_ref=sbuf.at[slot, d, f], dst_ref=rbuf.at[slot, d, f], send_sem=send_sems.at[slot, d, f],
            recv_sem=recv_sems.at[slot, d, f], device_id={"row": peer, "col": me_col}, device_id_type=MESH)
            for d, peer in enumerate((up, down))]

    def send(f, slot):
        for d, (r0, s) in enumerate(((halo, 0), (R - 2 * halo, 7))):
            for g in range(halo // 8):
                for c in range(NC):
                    sbuf[slot, d, f, g, c] = states[f][strided(r0 + 8 * g, c, s), :]
        for cp in copies(f, slot):
            cp.start()

    def receive(f, slot):
        for d, (r0, s) in enumerate(((R - halo, 7), (0, 0))):
            copies(f, slot)[d].wait()
            for g in range(halo // 8):
                for c in range(NC):
                    states[f][strided(r0 + 8 * g, c, s), :] = rbuf[slot, d, f, g, c]

    def after_exchange(t0, slot):
        at = [step(t0 + j, states[j % 2], states[1 - j % 2]) for j in range(AHEAD)]
        late = [(state_a, half + q) for q in range(half - half // 2)]
        for j in range(AHEAD):
            late = arc(at[j], halo + 1 + j, R - 2 * halo - 2 - 2 * j, 1, late)
        receive(1, slot)
        receive(0, slot)
        for r in (*range(halo), *range(R - halo, R)):
            edges(state_a, r)
        for j in range(AHEAD):
            late = arc(at[j], R - halo - 1 - j, 2 * halo + 2 + 2 * j, 1, late)
        for ref, r in late:
            edges(ref, r)

    def pair(i, _):
        level(2 * i, state_a, state_b)
        nth = (i + 1) * 2 // halo
        leave = (lax.rem(2 * i + 2, halo) == 0) & (2 * i + 2 < steps)

        @pl.when(i == 0)
        def _():
            convert(1)

        @pl.when(leave)
        def _():
            send(1, lax.rem(nth, 2))
        level(2 * i + 1, state_b, state_a)

        @pl.when(leave)
        def _():
            send(0, lax.rem(nth, 2))
        return 0

    phases = steps // halo

    def phase(p, _):
        @pl.when(p > 0)
        def _():
            after_exchange(p * halo, lax.rem(p, 2))
        lax.fori_loop(p * (halo // 2) + (p + phases - 1) // phases * (AHEAD // 2), (p + 1) * (halo // 2), pair, 0)
        return 0
    lax.fori_loop(0, phases, phase, 0)


def unpack_kernel(halo, a_ref, b_ref, u_hbm, v_hbm, raw, wide, sems):
    rows, cols = u_hbm.shape
    R = (rows + 2 * halo) // 8
    groups = [(r0, min(16, R - r0)) for r0 in range(0, R, 16)]
    copies = []
    for f, dst in enumerate((u_hbm, v_hbm)):
        for g, (r0, n) in enumerate(groups):
            for c in range(NC):
                parts = []
                for q in range(n):
                    at = pl.ds(((r0 + q) * NB + c + 1) * 8, 8)
                    if f == 0:
                        x = a_ref[at, :] * (1.0 / SCALE)
                    else:
                        x = (a_ref[at, :] - b_ref[at, :]) * (2.0 / SCALE)
                    parts.append(x)
                wide[f, g, pl.ds(c, 128, stride=NC), :8 * n] = jnp.concatenate(parts, axis=0).T
        for b in range(cols // 128):
            for g, (r0, n) in enumerate(groups):
                back = wide[f, g, pl.ds(b * 128, 128), :][:, :8 * n].T
                for q in range(n):
                    raw[f, b, pl.ds(r0 + q, 8, stride=R), :] = back[q * 8:q * 8 + 8, :]
            copies.append(pltpu.make_async_copy(raw.at[f, b, pl.ds(halo, rows), :], dst.at[:, pl.ds(b * 128, 128)],
                                                sems.at[f, b]))
            if len(copies) > 1:
                copies[-2].start()
    copies[-1].start()
    for cp in copies:
        cp.wait()


def solution(mesh):
    tile_spec = P(("ens", "row"), "col")

    def local_run(u_tile, v_tile, stencil_w):
        rows, cols = u_tile.shape
        steps = stencil_w.shape[0]
        halo = HALO
        R = (rows + 2 * halo) // 8
        nblk = cols // 128
        f32 = jnp.float32
        dma = pltpu.SemaphoreType.DMA
        raw = pltpu.VMEM((2, nblk + 1, 8 * R, 128), f32)
        wide = pltpu.VMEM((2, -(-R // 16), 128 * NC, 128), f32)
        vmem, hbm = pl.BlockSpec(memory_space=pltpu.VMEM), pl.BlockSpec(memory_space=pl.ANY)
        states = pl.pallas_call(
            functools.partial(kernel, steps, rows, cols, halo),
            out_shape=[jax.ShapeDtypeStruct((R * NB * 8, 128), f32)] * 2,
            in_specs=[hbm, hbm, hbm],
            out_specs=[vmem, vmem],
            scratch_shapes=[
                raw, pltpu.VMEM((2, rows, 128), f32), pltpu.VMEM((3, 3, steps), f32), pltpu.VMEM((5, steps, 128), f32), wide,
                pltpu.VMEM((2, 2, 2, halo // 8, NC, 8, 128), f32), pltpu.VMEM((2, 2, 2, halo // 8, NC, 8, 128), f32),
                dma((2, nblk)), dma((2, 2)), dma((2, 2, 2)), dma((2, 2, 2)), dma((2, 2, 2)), dma((2, 2, 2)), dma,
            ],
            compiler_params=pltpu.CompilerParams(collective_id=0, has_side_effects=True,
                                                 vmem_limit_bytes=44 * 1024 * 1024),
        )(*(pltpu.with_memory_space_constraint(x, pltpu.HBM) for x in (stencil_w.transpose(1, 2, 0), u_tile, v_tile)))
        return pl.pallas_call(
            functools.partial(unpack_kernel, halo),
            out_shape=[jax.ShapeDtypeStruct((rows, cols), f32)] * 2,
            in_specs=[vmem, vmem],
            out_specs=[hbm, hbm],
            scratch_shapes=[raw, wide, dma((2, nblk))],
            compiler_params=pltpu.CompilerParams(vmem_limit_bytes=32 * 1024 * 1024),
        )(*states)

    return jax.shard_map(local_run, mesh=mesh, in_specs=(tile_spec, tile_spec, P()), out_specs=(tile_spec, tile_spec), check_vma=False)
```

```python
import functools

import jax
import jax.numpy as jnp
from jax import lax
from jax.experimental import pallas as pl
from jax.experimental.pallas import tpu as pltpu
from jax.sharding import PartitionSpec as P

HALO = 16
AHEAD = 6
NC = 9
NB = 11
SCALE = 0.125
MESH = pl.DeviceIdType.MESH


def kernel(steps, rows, cols, halo, w_hbm, u_hbm, v_hbm, state_a, state_b,
           raw, gsend, w_ref, coef, wide, sbuf, rbuf,
           load_sem, col_sems, row_sems, diag_sems, send_sems, recv_sems, w_sem):
    R = (rows + 2 * halo) // 8
    nblk = cols // 128
    n_row = lax.axis_size("row")
    me_row, me_col = lax.axis_index("row"), lax.axis_index("col")
    up, down = lax.rem(me_row + n_row - 1, n_row), lax.rem(me_row + 1, n_row)
    other = 1 - me_col

    weights = pltpu.make_async_copy(w_hbm, w_ref, w_sem)
    weights.start()

    loads = []
    for f, src in enumerate((u_hbm, v_hbm)):
        for b in (0, nblk - 1, *range(1, nblk - 1)):
            cp = pltpu.make_async_copy(src.at[:, pl.ds(b * 128, 128)],
                                       raw.at[f, b, pl.ds(halo, rows), :], load_sem.at[f, b])
            cp.start()
            loads.append(cp)

    barrier = pltpu.get_barrier_semaphore()
    peers = [(up, me_col), (down, me_col), (me_row, other), (up, other), (down, other)]
    for r, c in peers:
        pl.semaphore_signal(barrier, inc=1, device_id={"row": r, "col": c}, device_id_type=MESH)

    states = (state_a, state_b)
    lane = lax.broadcasted_iota(jnp.int32, (64, 128), 1)

    def remote(src, dst, sems, r, c):
        cp = pltpu.make_async_remote_copy(src_ref=src, dst_ref=dst, send_sem=sems.at[0], recv_sem=sems.at[1],
                                          device_id={"row": r, "col": c}, device_id_type=MESH)
        cp.start()
        return cp

    halos = []
    for f in range(2):
        mine = loads[f * nblk:(f + 1) * nblk]
        mine[0].wait()
        mine[1].wait()

        def build(i, _, f=f):
            at = pl.multiple_of(i * 64, 64)
            gsend[f, pl.ds(at, 64), :] = jnp.where(lane < 64, raw[f, 0, pl.ds(halo + at, 64), :],
                                                   raw[f, nblk - 1, pl.ds(halo + at, 64), :])
            return 0
        lax.fori_loop(0, rows // 64, build, 0)
        if f == 0:
            pl.semaphore_wait(barrier, len(peers))
        cols_in = [
            remote(gsend.at[f], raw.at[f, nblk, pl.ds(halo, rows), :], col_sems.at[f], me_row, other),
            remote(gsend.at[f, pl.ds(0, halo), :], raw.at[f, nblk, pl.ds(halo + rows, halo), :],
                   diag_sems.at[f, 0], up, other),
            remote(gsend.at[f, pl.ds(rows - halo, halo), :], raw.at[f, nblk, pl.ds(0, halo), :],
                   diag_sems.at[f, 1], down, other)]
        for cp in mine[2:]:
            cp.wait()
        rows_in = [
            remote(raw.at[f, pl.ds(0, nblk), pl.ds(halo, halo), :],
                   raw.at[f, pl.ds(0, nblk), pl.ds(halo + rows, halo), :], row_sems.at[f, 0], up, me_col),
            remote(raw.at[f, pl.ds(0, nblk), pl.ds(rows, halo), :],
                   raw.at[f, pl.ds(0, nblk), pl.ds(0, halo), :], row_sems.at[f, 1], down, me_col)]
        halos.append((rows_in, cols_in))

    weights.wait()
    w = lambda i, j: w_ref[i, j:j + 1, :]
    for k, row in enumerate((0.25 * (w(0, 0) + w(0, 2)), 0.25 * (w(0, 2) - w(0, 0)), 0.5 * w(0, 1),
                              0.5 * w(1, 0), 1.5 + 0.5 * w(1, 1))):
        coef[k] = jnp.broadcast_to(row, (128, steps)).T

    groups = R // 16
    spare = R % 16

    def reg(r, c):
        return pl.ds(pl.multiple_of((r * NB + c + 1) * 8, 8), 8)

    def line(r, shift=0):
        return pl.ds(pl.multiple_of((r * NB + 1 + shift) * 8, 8), NC * 8)

    def in_registers(base, q, c):
        return pl.ds(pl.multiple_of(base + (q * NB + c + 1) * 8, 8), 8)

    def to_lanes(f, i, n, blocks):
        r0 = i * 16
        for b in blocks:
            x = jnp.concatenate([raw[f, b, pl.ds(r0 + q, 8, stride=R), :] for q in range(n)], axis=0)
            wide[f, i, pl.ds(b * 128, 128), :8 * n] = (x * (0.5 * SCALE if f else SCALE)).T

    def to_registers(f, i, n):
        base = i * (16 * NB * 8)
        for c in range(NC):
            back = wide[f, i, pl.ds(c, 128, stride=NC), :][:, :8 * n].T
            if f == 1:
                back = jnp.concatenate([state_b[in_registers(base, q, c), :] for q in range(n)], axis=0) + back
            puts = [(c, back)]
            if c == 0:
                puts.append((NC, pltpu.roll(back, 127, 1)))
            if c == NC - 1:
                puts.append((-1, pltpu.roll(back, 1, 1)))
            for to, x in puts:
                for q in range(n):
                    states[f][in_registers(base, q, to), :] = x[q * 8:q * 8 + 8, :]

    def over_groups(fn):
        lax.fori_loop(0, groups, lambda i, _: (fn(i, 16), 0)[1], 0)
        if spare:
            fn(groups, spare)

    def convert(f):
        for cp in halos[f][0]:
            cp.wait()
        over_groups(lambda i, n: to_lanes(f, i, n, range(nblk)))
        for cp in halos[f][1]:
            cp.wait()
        for i in range(groups):
            to_lanes(f, i, 16, (nblk,))
        if spare:
            to_lanes(f, groups, spare, (nblk,))
        over_groups(lambda i, n: to_registers(f, i, n))

    convert(0)

    def same(r, _):
        state_b[line(r), :] = state_a[line(r), :]
        return 0
    lax.fori_loop(0, R, same, 0)

    def step(t, cur, new):
        alpha, beta, side, mid_s, centre = (
            jnp.broadcast_to(coef[k, pl.ds(t, 1), :], (NC * 8, 128)) for k in range(5))

        def contrib(r):
            left, here, right = cur[line(r, -1), :], cur[line(r), :], cur[pl.ds((r * NB + 2) * 8, NC * 8), :]
            s, d = left + right, right - left
            e, bd = alpha * s + side * here, beta * d
            return e + bd, mid_s * s + centre * here, e - bd

        def store(r, x):
            at = pl.ds((r * NB + 1) * 8, NC * 8)
            new[at, :] = x - new[at, :]
        return contrib, store, new

    def edges(ref, r):
        at = lambda c: pl.ds((r * NB + c + 1) * 8, 8)
        ref[at(NC), :] = pltpu.roll(ref[at(0), :], 127, 1)
        ref[at(-1), :] = pltpu.roll(ref[at(NC - 1), :], 1, 1)

    def turn(x, by):
        return jnp.concatenate([pltpu.roll(x[8 * c:8 * c + 8, :], by, 0) for c in range(NC)], axis=0)

    def cross(x, r, to):
        if (r, to) == (R - 1, 0):
            return turn(x, 1)
        return turn(x, 7) if (r, to) == (0, R - 1) else x

    def arc(at, first, count, way, late):
        contrib, store, new = at
        fwd, back = (0, 2) if way > 0 else (2, 0)
        before, r = (first - way) % R, first % R
        here = contrib(r)
        away, acc = here[fwd], cross(contrib(before)[fwd], before, r) + here[1]
        for n in (count // 3, count // 3, count - 2 * (count // 3)):
            for ref, row in late:
                edges(ref, row)
            late = []
            for _ in range(n):
                to = (r + way) % R
                nxt = contrib(to)
                store(r, acc + cross(nxt[back], to, r))
                away, acc = nxt[fwd], cross(away, r, to) + nxt[1]
                late.append((new, r))
                r = to
        return late

    half = R // 2

    def level(t, cur, new):
        at = step(t, cur, new)
        late = arc(at, 0, half, 1, [(cur, half + q) for q in range(half - 2 * (half // 3))])
        arc(at, R - 1, R - half, -1, late)

    def strided(r, c, s):
        return pl.ds((r * NB + c + 1) * 8 + s, 8, stride=NB * 8)

    def copies(f, slot):
        return [pltpu.make_async_remote_copy(
            src_ref=sbuf.at[slot, d, f], dst_ref=rbuf.at[slot, d, f], send_sem=send_sems.at[slot, d, f],
            recv_sem=recv_sems.at[slot, d, f], device_id={"row": peer, "col": me_col}, device_id_type=MESH)
            for d, peer in enumerate((up, down))]

    def send(f, slot):
        for d, (r0, s) in enumerate(((halo, 0), (R - 2 * halo, 7))):
            for g in range(halo // 8):
                for c in range(NC):
                    sbuf[slot, d, f, g, c] = states[f][strided(r0 + 8 * g, c, s), :]
        for cp in copies(f, slot):
            cp.start()

    def receive(f, slot):
        for d, (r0, s) in enumerate(((R - halo, 7), (0, 0))):
            copies(f, slot)[d].wait()
            for g in range(halo // 8):
                for c in range(NC):
                    states[f][strided(r0 + 8 * g, c, s), :] = rbuf[slot, d, f, g, c]

    def after_exchange(t0, slot):
        at = [step(t0 + j, states[j % 2], states[1 - j % 2]) for j in range(AHEAD)]
        late = [(state_a, half + q) for q in range(half - 2 * (half // 3))]
        for j in range(AHEAD):
            late = arc(at[j], halo + 1 + j, R - 2 * halo - 2 - 2 * j, 1, late)
        receive(1, slot)
        receive(0, slot)
        for r in (*range(halo), *range(R - halo, R)):
            edges(state_a, r)
        for j in range(AHEAD):
            late = arc(at[j], R - halo - 1 - j, 2 * halo + 2 + 2 * j, 1, late)
        for ref, r in late:
            edges(ref, r)

    def pair(i, _):
        level(2 * i, state_a, state_b)
        nth = (i + 1) * 2 // halo
        leave = (lax.rem(2 * i + 2, halo) == 0) & (2 * i + 2 < steps)

        @pl.when(i == 0)
        def _():
            convert(1)

        @pl.when(leave)
        def _():
            send(1, lax.rem(nth, 2))
        level(2 * i + 1, state_b, state_a)

        @pl.when(leave)
        def _():
            send(0, lax.rem(nth, 2))
        return 0

    phases = steps // halo

    def phase(p, _):
        @pl.when(p > 0)
        def _():
            after_exchange(p * halo, lax.rem(p, 2))
        lax.fori_loop(p * (halo // 2) + (p + phases - 1) // phases * (AHEAD // 2), (p + 1) * (halo // 2), pair, 0)
        return 0
    lax.fori_loop(0, phases, phase, 0)


def unpack_kernel(halo, a_ref, b_ref, u_hbm, v_hbm, raw, wide, sems):
    rows, cols = u_hbm.shape
    R = (rows + 2 * halo) // 8
    groups = [(r0, min(16, R - r0)) for r0 in range(0, R, 16)]
    copies = []
    for f, dst in enumerate((u_hbm, v_hbm)):
        for g, (r0, n) in enumerate(groups):
            for c in range(NC):
                parts = []
                for q in range(n):
                    at = pl.ds(((r0 + q) * NB + c + 1) * 8, 8)
                    if f == 0:
                        x = a_ref[at, :] * (1.0 / SCALE)
                    else:
                        x = (a_ref[at, :] - b_ref[at, :]) * (2.0 / SCALE)
                    parts.append(x)
                wide[f, g, pl.ds(c, 128, stride=NC), :8 * n] = jnp.concatenate(parts, axis=0).T
        for b in range(cols // 128):
            for g, (r0, n) in enumerate(groups):
                back = wide[f, g, pl.ds(b * 128, 128), :][:, :8 * n].T
                for q in range(n):
                    raw[f, b, pl.ds(r0 + q, 8, stride=R), :] = back[q * 8:q * 8 + 8, :]
            copies.append(pltpu.make_async_copy(raw.at[f, b, pl.ds(halo, rows), :], dst.at[:, pl.ds(b * 128, 128)],
                                                sems.at[f, b]))
            if len(copies) > 1:
                copies[-2].start()
    copies[-1].start()
    for cp in copies:
        cp.wait()


def solution(mesh):
    tile_spec = P(("ens", "row"), "col")

    def local_run(u_tile, v_tile, stencil_w):
        rows, cols = u_tile.shape
        steps = stencil_w.shape[0]
        halo = HALO
        R = (rows + 2 * halo) // 8
        nblk = cols // 128
        f32 = jnp.float32
        dma = pltpu.SemaphoreType.DMA
        raw = pltpu.VMEM((2, nblk + 1, 8 * R, 128), f32)
        wide = pltpu.VMEM((2, -(-R // 16), 128 * NC, 128), f32)
        vmem, hbm = pl.BlockSpec(memory_space=pltpu.VMEM), pl.BlockSpec(memory_space=pl.ANY)
        states = pl.pallas_call(
            functools.partial(kernel, steps, rows, cols, halo),
            out_shape=[jax.ShapeDtypeStruct((R * NB * 8, 128), f32)] * 2,
            in_specs=[hbm, hbm, hbm],
            out_specs=[vmem, vmem],
            scratch_shapes=[
                raw, pltpu.VMEM((2, rows, 128), f32), pltpu.VMEM((3, 3, steps), f32), pltpu.VMEM((5, steps, 128), f32), wide,
                pltpu.VMEM((2, 2, 2, halo // 8, NC, 8, 128), f32), pltpu.VMEM((2, 2, 2, halo // 8, NC, 8, 128), f32),
                dma((2, nblk)), dma((2, 2)), dma((2, 2, 2)), dma((2, 2, 2)), dma((2, 2, 2)), dma((2, 2, 2)), dma,
            ],
            compiler_params=pltpu.CompilerParams(collective_id=0, has_side_effects=True,
                                                 vmem_limit_bytes=44 * 1024 * 1024),
        )(*(pltpu.with_memory_space_constraint(x, pltpu.HBM) for x in (stencil_w.transpose(1, 2, 0), u_tile, v_tile)))
        return pl.pallas_call(
            functools.partial(unpack_kernel, halo),
            out_shape=[jax.ShapeDtypeStruct((rows, cols), f32)] * 2,
            in_specs=[vmem, vmem],
            out_specs=[hbm, hbm],
            scratch_shapes=[raw, wide, dma((2, nblk))],
            compiler_params=pltpu.CompilerParams(vmem_limit_bytes=32 * 1024 * 1024),
        )(*states)

    return jax.shard_map(local_run, mesh=mesh, in_specs=(tile_spec, tile_spec, P()), out_specs=(tile_spec, tile_spec), check_vma=False)
```

```python
import functools

import jax
import jax.numpy as jnp
from jax import lax
from jax.experimental import pallas as pl
from jax.experimental.pallas import tpu as pltpu
from jax.sharding import PartitionSpec as P

HALO = 16
AHEAD = 6
NC = 9
NB = 11
SCALE = 0.125
MESH = pl.DeviceIdType.MESH


def kernel(steps, rows, cols, halo, w_hbm, u_hbm, v_hbm, state_a, state_b,
           raw, gsend, w_ref, coef, wide, sbuf, rbuf,
           load_sem, col_sems, row_sems, diag_sems, send_sems, recv_sems, w_sem):
    R = (rows + 2 * halo) // 8
    nblk = cols // 128
    n_row = lax.axis_size("row")
    me_row, me_col = lax.axis_index("row"), lax.axis_index("col")
    up, down = lax.rem(me_row + n_row - 1, n_row), lax.rem(me_row + 1, n_row)
    other = 1 - me_col

    weights = pltpu.make_async_copy(w_hbm, w_ref, w_sem)
    weights.start()

    loads = []
    for f, src in enumerate((u_hbm, v_hbm)):
        for b in (0, nblk - 1, *range(1, nblk - 1)):
            cp = pltpu.make_async_copy(src.at[:, pl.ds(b * 128, 128)],
                                       raw.at[f, b, pl.ds(halo, rows), :], load_sem.at[f, b])
            cp.start()
            loads.append(cp)

    barrier = pltpu.get_barrier_semaphore()
    peers = [(up, me_col), (down, me_col), (me_row, other), (up, other), (down, other)]
    for r, c in peers:
        pl.semaphore_signal(barrier, inc=1, device_id={"row": r, "col": c}, device_id_type=MESH)

    states = (state_a, state_b)
    lane = lax.broadcasted_iota(jnp.int32, (64, 128), 1)

    def remote(src, dst, sems, r, c):
        cp = pltpu.make_async_remote_copy(src_ref=src, dst_ref=dst, send_sem=sems.at[0], recv_sem=sems.at[1],
                                          device_id={"row": r, "col": c}, device_id_type=MESH)
        cp.start()
        return cp

    halos = []
    for f in range(2):
        mine = loads[f * nblk:(f + 1) * nblk]
        mine[0].wait()
        mine[1].wait()

        def build(i, _, f=f):
            at = pl.multiple_of(i * 64, 64)
            gsend[f, pl.ds(at, 64), :] = jnp.where(lane < 64, raw[f, 0, pl.ds(halo + at, 64), :],
                                                   raw[f, nblk - 1, pl.ds(halo + at, 64), :])
            return 0
        lax.fori_loop(0, rows // 64, build, 0)
        if f == 0:
            pl.semaphore_wait(barrier, len(peers))
        cols_in = [
            remote(gsend.at[f], raw.at[f, nblk, pl.ds(halo, rows), :], col_sems.at[f], me_row, other),
            remote(gsend.at[f, pl.ds(0, halo), :], raw.at[f, nblk, pl.ds(halo + rows, halo), :],
                   diag_sems.at[f, 0], up, other),
            remote(gsend.at[f, pl.ds(rows - halo, halo), :], raw.at[f, nblk, pl.ds(0, halo), :],
                   diag_sems.at[f, 1], down, other)]
        for cp in mine[2:]:
            cp.wait()
        rows_in = [
            remote(raw.at[f, pl.ds(0, nblk), pl.ds(halo, halo), :],
                   raw.at[f, pl.ds(0, nblk), pl.ds(halo + rows, halo), :], row_sems.at[f, 0], up, me_col),
            remote(raw.at[f, pl.ds(0, nblk), pl.ds(rows, halo), :],
                   raw.at[f, pl.ds(0, nblk), pl.ds(0, halo), :], row_sems.at[f, 1], down, me_col)]
        halos.append((rows_in, cols_in))

    weights.wait()
    w = lambda i, j: w_ref[i, j:j + 1, :]
    for k, row in enumerate((0.25 * (w(0, 0) + w(0, 2)), 0.25 * (w(0, 2) - w(0, 0)), 0.5 * w(0, 1),
                              0.5 * w(1, 0), 1.5 + 0.5 * w(1, 1))):
        coef[k] = jnp.broadcast_to(row, (128, steps)).T

    groups = R // 16
    spare = R % 16

    def reg(r, c):
        return pl.ds(pl.multiple_of((r * NB + c + 1) * 8, 8), 8)

    def line(r, shift=0):
        return pl.ds(pl.multiple_of((r * NB + 1 + shift) * 8, 8), NC * 8)

    def in_registers(base, q, c):
        return pl.ds(pl.multiple_of(base + (q * NB + c + 1) * 8, 8), 8)

    def to_lanes(f, i, n, blocks):
        r0 = i * 16
        for b in blocks:
            x = jnp.concatenate([raw[f, b, pl.ds(r0 + q, 8, stride=R), :] for q in range(n)], axis=0)
            wide[f, i, pl.ds(b * 128, 128), :8 * n] = (x * (0.5 * SCALE if f else SCALE)).T

    def to_registers(f, i, n):
        base = i * (16 * NB * 8)
        for c in range(NC):
            back = wide[f, i, pl.ds(c, 128, stride=NC), :][:, :8 * n].T
            if f == 1:
                back = jnp.concatenate([state_b[in_registers(base, q, c), :] for q in range(n)], axis=0) + back
            puts = [(c, back)]
            if c == 0:
                puts.append((NC, pltpu.roll(back, 127, 1)))
            if c == NC - 1:
                puts.append((-1, pltpu.roll(back, 1, 1)))
            for to, x in puts:
                for q in range(n):
                    states[f][in_registers(base, q, to), :] = x[q * 8:q * 8 + 8, :]

    def over_groups(fn):
        lax.fori_loop(0, groups, lambda i, _: (fn(i, 16), 0)[1], 0)
        if spare:
            fn(groups, spare)

    def convert(f):
        for cp in halos[f][0]:
            cp.wait()
        over_groups(lambda i, n: to_lanes(f, i, n, range(nblk)))
        for cp in halos[f][1]:
            cp.wait()
        for i in range(groups):
            to_lanes(f, i, 16, (nblk,))
        if spare:
            to_lanes(f, groups, spare, (nblk,))
        over_groups(lambda i, n: to_registers(f, i, n))

    convert(0)

    def same(r, _):
        state_b[line(r), :] = state_a[line(r), :]
        return 0
    lax.fori_loop(0, R, same, 0)

    def step(t, cur, new):
        alpha, beta, side, mid_s, centre = (
            jnp.broadcast_to(coef[k, pl.ds(t, 1), :], (NC * 8, 128)) for k in range(5))

        def contrib(r):
            left, here, right = cur[line(r, -1), :], cur[line(r), :], cur[pl.ds((r * NB + 2) * 8, NC * 8), :]
            s, d = left + right, right - left
            bd, e = beta * d, side * here + alpha * s
            return e + bd, centre * here + mid_s * s, e - bd

        def store(r, x):
            at = pl.ds((r * NB + 1) * 8, NC * 8)
            new[at, :] = x - new[at, :]
        return contrib, store, new

    def edges(ref, r):
        at = lambda c: pl.ds((r * NB + c + 1) * 8, 8)
        ref[at(NC), :] = pltpu.roll(ref[at(0), :], 127, 1)
        ref[at(-1), :] = pltpu.roll(ref[at(NC - 1), :], 1, 1)

    def turn(x, by):
        return jnp.concatenate([pltpu.roll(x[8 * c:8 * c + 8, :], by, 0) for c in range(NC)], axis=0)

    def cross(x, r, to):
        if (r, to) == (R - 1, 0):
            return turn(x, 1)
        return turn(x, 7) if (r, to) == (0, R - 1) else x

    def arc(at, first, count, way, late):
        contrib, store, new = at
        fwd, back = (0, 2) if way > 0 else (2, 0)
        before, r = (first - way) % R, first % R
        here = contrib(r)
        away, acc = here[fwd], cross(contrib(before)[fwd], before, r) + here[1]
        for n in (count // 3, count // 3, count - 2 * (count // 3)):
            for ref, row in late:
                edges(ref, row)
            late = []
            for _ in range(n):
                to = (r + way) % R
                nxt = contrib(to)
                store(r, acc + cross(nxt[back], to, r))
                away, acc = nxt[fwd], cross(away, r, to) + nxt[1]
                late.append((new, r))
                r = to
        return late

    half = R // 2

    def level(t, cur, new):
        at = step(t, cur, new)
        late = arc(at, 0, half, 1, [(cur, half + q) for q in range(half - 2 * (half // 3))])
        arc(at, R - 1, R - half, -1, late)

    def strided(r, c, s):
        return pl.ds((r * NB + c + 1) * 8 + s, 8, stride=NB * 8)

    def copies(f, slot):
        return [pltpu.make_async_remote_copy(
            src_ref=sbuf.at[slot, d, f], dst_ref=rbuf.at[slot, d, f], send_sem=send_sems.at[slot, d, f],
            recv_sem=recv_sems.at[slot, d, f], device_id={"row": peer, "col": me_col}, device_id_type=MESH)
            for d, peer in enumerate((up, down))]

    def send(f, slot):
        for d, (r0, s) in enumerate(((halo, 0), (R - 2 * halo, 7))):
            for g in range(halo // 8):
                for c in range(NC):
                    sbuf[slot, d, f, g, c] = states[f][strided(r0 + 8 * g, c, s), :]
        for cp in copies(f, slot):
            cp.start()

    def receive(f, slot):
        for d, (r0, s) in enumerate(((R - halo, 7), (0, 0))):
            copies(f, slot)[d].wait()
            for g in range(halo // 8):
                for c in range(NC):
                    states[f][strided(r0 + 8 * g, c, s), :] = rbuf[slot, d, f, g, c]

    def after_exchange(t0, slot):
        at = [step(t0 + j, states[j % 2], states[1 - j % 2]) for j in range(AHEAD)]
        late = [(state_a, half + q) for q in range(half - 2 * (half // 3))]
        for j in range(AHEAD):
            late = arc(at[j], halo + 1 + j, R - 2 * halo - 2 - 2 * j, 1, late)
        receive(1, slot)
        receive(0, slot)
        for r in (*range(halo), *range(R - halo, R)):
            edges(state_a, r)
        for j in range(AHEAD):
            late = arc(at[j], R - halo - 1 - j, 2 * halo + 2 + 2 * j, 1, late)
        for ref, r in late:
            edges(ref, r)

    def pair(i, _):
        level(2 * i, state_a, state_b)
        nth = (i + 1) * 2 // halo
        leave = (lax.rem(2 * i + 2, halo) == 0) & (2 * i + 2 < steps)

        @pl.when(i == 0)
        def _():
            convert(1)

        @pl.when(leave)
        def _():
            send(1, lax.rem(nth, 2))
        level(2 * i + 1, state_b, state_a)

        @pl.when(leave)
        def _():
            send(0, lax.rem(nth, 2))
        return 0

    phases = steps // halo

    def phase(p, _):
        @pl.when(p > 0)
        def _():
            after_exchange(p * halo, lax.rem(p, 2))
        lax.fori_loop(p * (halo // 2) + (p + phases - 1) // phases * (AHEAD // 2), (p + 1) * (halo // 2), pair, 0)
        return 0
    lax.fori_loop(0, phases, phase, 0)


def unpack_kernel(halo, a_ref, b_ref, u_hbm, v_hbm, raw, wide, sems):
    rows, cols = u_hbm.shape
    R = (rows + 2 * halo) // 8
    groups = [(r0, min(16, R - r0)) for r0 in range(0, R, 16)]
    copies = []
    for f, dst in enumerate((u_hbm, v_hbm)):
        for g, (r0, n) in enumerate(groups):
            for c in range(NC):
                parts = []
                for q in range(n):
                    at = pl.ds(((r0 + q) * NB + c + 1) * 8, 8)
                    if f == 0:
                        x = a_ref[at, :] * (1.0 / SCALE)
                    else:
                        x = (a_ref[at, :] - b_ref[at, :]) * (2.0 / SCALE)
                    parts.append(x)
                wide[f, g, pl.ds(c, 128, stride=NC), :8 * n] = jnp.concatenate(parts, axis=0).T
        for b in range(cols // 128):
            for g, (r0, n) in enumerate(groups):
                back = wide[f, g, pl.ds(b * 128, 128), :][:, :8 * n].T
                for q in range(n):
                    raw[f, b, pl.ds(r0 + q, 8, stride=R), :] = back[q * 8:q * 8 + 8, :]
            copies.append(pltpu.make_async_copy(raw.at[f, b, pl.ds(halo, rows), :], dst.at[:, pl.ds(b * 128, 128)],
                                                sems.at[f, b]))
            if len(copies) > 1:
                copies[-2].start()
    copies[-1].start()
    for cp in copies:
        cp.wait()


def solution(mesh):
    tile_spec = P(("ens", "row"), "col")

    def local_run(u_tile, v_tile, stencil_w):
        rows, cols = u_tile.shape
        steps = stencil_w.shape[0]
        halo = HALO
        R = (rows + 2 * halo) // 8
        nblk = cols // 128
        f32 = jnp.float32
        dma = pltpu.SemaphoreType.DMA
        raw = pltpu.VMEM((2, nblk + 1, 8 * R, 128), f32)
        wide = pltpu.VMEM((2, -(-R // 16), 128 * NC, 128), f32)
        vmem, hbm = pl.BlockSpec(memory_space=pltpu.VMEM), pl.BlockSpec(memory_space=pl.ANY)
        states = pl.pallas_call(
            functools.partial(kernel, steps, rows, cols, halo),
            out_shape=[jax.ShapeDtypeStruct((R * NB * 8, 128), f32)] * 2,
            in_specs=[hbm, hbm, hbm],
            out_specs=[vmem, vmem],
            scratch_shapes=[
                raw, pltpu.VMEM((2, rows, 128), f32), pltpu.VMEM((3, 3, steps), f32), pltpu.VMEM((5, steps, 128), f32), wide,
                pltpu.VMEM((2, 2, 2, halo // 8, NC, 8, 128), f32), pltpu.VMEM((2, 2, 2, halo // 8, NC, 8, 128), f32),
                dma((2, nblk)), dma((2, 2)), dma((2, 2, 2)), dma((2, 2, 2)), dma((2, 2, 2)), dma((2, 2, 2)), dma,
            ],
            compiler_params=pltpu.CompilerParams(collective_id=0, has_side_effects=True,
                                                 vmem_limit_bytes=44 * 1024 * 1024),
        )(*(pltpu.with_memory_space_constraint(x, pltpu.HBM) for x in (stencil_w.transpose(1, 2, 0), u_tile, v_tile)))
        return pl.pallas_call(
            functools.partial(unpack_kernel, halo),
            out_shape=[jax.ShapeDtypeStruct((rows, cols), f32)] * 2,
            in_specs=[vmem, vmem],
            out_specs=[hbm, hbm],
            scratch_shapes=[raw, wide, dma((2, nblk))],
            compiler_params=pltpu.CompilerParams(vmem_limit_bytes=32 * 1024 * 1024),
        )(*states)

    return jax.shard_map(local_run, mesh=mesh, in_specs=(tile_spec, tile_spec, P()), out_specs=(tile_spec, tile_spec), check_vma=False)
```

```python
import functools

import jax
import jax.numpy as jnp
from jax import lax
from jax.experimental import pallas as pl
from jax.experimental.pallas import tpu as pltpu
from jax.sharding import PartitionSpec as P

HALO = 16
AHEAD = 6
NC = 9
NB = 11
SCALE = 0.125
MESH = pl.DeviceIdType.MESH


def kernel(steps, rows, cols, halo, w_hbm, u_hbm, v_hbm, state_a, state_b,
           raw, gsend, w_ref, coef, wide, sbuf, rbuf,
           load_sem, col_sems, row_sems, diag_sems, send_sems, recv_sems, w_sem):
    R = (rows + 2 * halo) // 8
    nblk = cols // 128
    n_row = lax.axis_size("row")
    me_row, me_col = lax.axis_index("row"), lax.axis_index("col")
    up, down = lax.rem(me_row + n_row - 1, n_row), lax.rem(me_row + 1, n_row)
    other = 1 - me_col

    weights = pltpu.make_async_copy(w_hbm, w_ref, w_sem)
    weights.start()

    loads = []
    for f, src in enumerate((u_hbm, v_hbm)):
        for b in (0, nblk - 1, *range(1, nblk - 1)):
            cp = pltpu.make_async_copy(src.at[:, pl.ds(b * 128, 128)],
                                       raw.at[f, b, pl.ds(halo, rows), :], load_sem.at[f, b])
            cp.start()
            loads.append(cp)

    barrier = pltpu.get_barrier_semaphore()
    peers = [(up, me_col), (down, me_col), (me_row, other), (up, other), (down, other)]
    for r, c in peers:
        pl.semaphore_signal(barrier, inc=1, device_id={"row": r, "col": c}, device_id_type=MESH)

    states = (state_a, state_b)
    lane = lax.broadcasted_iota(jnp.int32, (64, 128), 1)

    def remote(src, dst, sems, r, c):
        cp = pltpu.make_async_remote_copy(src_ref=src, dst_ref=dst, send_sem=sems.at[0], recv_sem=sems.at[1],
                                          device_id={"row": r, "col": c}, device_id_type=MESH)
        cp.start()
        return cp

    halos = []
    for f in range(2):
        mine = loads[f * nblk:(f + 1) * nblk]
        mine[0].wait()
        mine[1].wait()

        def build(i, _, f=f):
            at = pl.multiple_of(i * 64, 64)
            gsend[f, pl.ds(at, 64), :] = jnp.where(lane < 64, raw[f, 0, pl.ds(halo + at, 64), :],
                                                   raw[f, nblk - 1, pl.ds(halo + at, 64), :])
            return 0
        lax.fori_loop(0, rows // 64, build, 0)
        if f == 0:
            pl.semaphore_wait(barrier, len(peers))
        cols_in = [
            remote(gsend.at[f], raw.at[f, nblk, pl.ds(halo, rows), :], col_sems.at[f], me_row, other),
            remote(gsend.at[f, pl.ds(0, halo), :], raw.at[f, nblk, pl.ds(halo + rows, halo), :],
                   diag_sems.at[f, 0], up, other),
            remote(gsend.at[f, pl.ds(rows - halo, halo), :], raw.at[f, nblk, pl.ds(0, halo), :],
                   diag_sems.at[f, 1], down, other)]
        for cp in mine[2:]:
            cp.wait()
        rows_in = [
            remote(raw.at[f, pl.ds(0, nblk), pl.ds(halo, halo), :],
                   raw.at[f, pl.ds(0, nblk), pl.ds(halo + rows, halo), :], row_sems.at[f, 0], up, me_col),
            remote(raw.at[f, pl.ds(0, nblk), pl.ds(rows, halo), :],
                   raw.at[f, pl.ds(0, nblk), pl.ds(0, halo), :], row_sems.at[f, 1], down, me_col)]
        halos.append((rows_in, cols_in))

    weights.wait()
    w = lambda i, j: w_ref[i, j:j + 1, :]
    for k, row in enumerate((0.25 * (w(0, 0) + w(0, 2)), 0.25 * (w(0, 2) - w(0, 0)), 0.5 * w(0, 1),
                              0.5 * w(1, 0), 1.5 + 0.5 * w(1, 1))):
        coef[k] = jnp.broadcast_to(row, (128, steps)).T

    groups = R // 16
    spare = R % 16

    def reg(r, c):
        return pl.ds(pl.multiple_of((r * NB + c + 1) * 8, 8), 8)

    def line(r, shift=0):
        return pl.ds(pl.multiple_of((r * NB + 1 + shift) * 8, 8), NC * 8)

    def in_registers(base, q, c):
        return pl.ds(pl.multiple_of(base + (q * NB + c + 1) * 8, 8), 8)

    def to_lanes(f, i, n, blocks):
        r0 = i * 16
        for b in blocks:
            x = jnp.concatenate([raw[f, b, pl.ds(r0 + q, 8, stride=R), :] for q in range(n)], axis=0)
            wide[f, i, pl.ds(b * 128, 128), :8 * n] = (x * (0.5 * SCALE if f else SCALE)).T

    def to_registers(f, i, n):
        base = i * (16 * NB * 8)
        for c in range(NC):
            back = wide[f, i, pl.ds(c, 128, stride=NC), :][:, :8 * n].T
            if f == 1:
                back = jnp.concatenate([state_b[in_registers(base, q, c), :] for q in range(n)], axis=0) + back
            puts = [(c, back)]
            if c == 0:
                puts.append((NC, pltpu.roll(back, 127, 1)))
            if c == NC - 1:
                puts.append((-1, pltpu.roll(back, 1, 1)))
            for to, x in puts:
                for q in range(n):
                    states[f][in_registers(base, q, to), :] = x[q * 8:q * 8 + 8, :]

    def over_groups(fn):
        lax.fori_loop(0, groups, lambda i, _: (fn(i, 16), 0)[1], 0)
        if spare:
            fn(groups, spare)

    def convert(f):
        for cp in halos[f][0]:
            cp.wait()
        over_groups(lambda i, n: to_lanes(f, i, n, range(nblk)))
        for cp in halos[f][1]:
            cp.wait()
        for i in range(groups):
            to_lanes(f, i, 16, (nblk,))
        if spare:
            to_lanes(f, groups, spare, (nblk,))
        over_groups(lambda i, n: to_registers(f, i, n))

    convert(0)

    def same(r, _):
        state_b[line(r), :] = state_a[line(r), :]
        return 0
    lax.fori_loop(0, R, same, 0)

    def step(t, cur, new):
        alpha, beta, side, mid_s, centre = (
            jnp.broadcast_to(coef[k, pl.ds(t, 1), :], (NC * 8, 128)) for k in range(5))

        def contrib(r):
            left, here, right = cur[line(r, -1), :], cur[line(r), :], cur[pl.ds((r * NB + 2) * 8, NC * 8), :]
            s, d = left + right, right - left
            bd, e = beta * d, side * here + alpha * s
            return e + bd, centre * here + mid_s * s, e - bd

        def store(r, x):
            at = pl.ds((r * NB + 1) * 8, NC * 8)
            new[at, :] = x - new[at, :]
        return contrib, store, new

    def edges(ref, r):
        at = lambda c: pl.ds((r * NB + c + 1) * 8, 8)
        ref[at(NC), :] = pltpu.roll(ref[at(0), :], 127, 1)
        ref[at(-1), :] = pltpu.roll(ref[at(NC - 1), :], 1, 1)

    def turn(x, by):
        return jnp.concatenate([pltpu.roll(x[8 * c:8 * c + 8, :], by, 0) for c in range(NC)], axis=0)

    def cross(x, r, to):
        if (r, to) == (R - 1, 0):
            return turn(x, 1)
        return turn(x, 7) if (r, to) == (0, R - 1) else x

    def arc(at, first, count, way, late):
        contrib, store, new = at
        fwd, back = (0, 2) if way > 0 else (2, 0)
        before, r = (first - way) % R, first % R
        here = contrib(r)
        away, acc = here[fwd], cross(contrib(before)[fwd], before, r) + here[1]
        for n in (*[count // 4] * 3, count - 3 * (count // 4)):
            for ref, row in late:
                edges(ref, row)
            late = []
            for _ in range(n):
                to = (r + way) % R
                nxt = contrib(to)
                store(r, acc + cross(nxt[back], to, r))
                away, acc = nxt[fwd], cross(away, r, to) + nxt[1]
                late.append((new, r))
                r = to
        return late

    half = R // 2

    def level(t, cur, new):
        at = step(t, cur, new)
        late = arc(at, 0, half, 1, [(cur, half + q) for q in range(half - 3 * (half // 4))])
        arc(at, R - 1, R - half, -1, late)

    def strided(r, c, s):
        return pl.ds((r * NB + c + 1) * 8 + s, 8, stride=NB * 8)

    def copies(f, slot):
        return [pltpu.make_async_remote_copy(
            src_ref=sbuf.at[slot, d, f], dst_ref=rbuf.at[slot, d, f], send_sem=send_sems.at[slot, d, f],
            recv_sem=recv_sems.at[slot, d, f], device_id={"row": peer, "col": me_col}, device_id_type=MESH)
            for d, peer in enumerate((up, down))]

    def send(f, slot):
        for d, (r0, s) in enumerate(((halo, 0), (R - 2 * halo, 7))):
            for g in range(halo // 8):
                for c in range(NC):
                    sbuf[slot, d, f, g, c] = states[f][strided(r0 + 8 * g, c, s), :]
        for cp in copies(f, slot):
            cp.start()

    def receive(f, slot):
        for d, (r0, s) in enumerate(((R - halo, 7), (0, 0))):
            copies(f, slot)[d].wait()
            for g in range(halo // 8):
                for c in range(NC):
                    states[f][strided(r0 + 8 * g, c, s), :] = rbuf[slot, d, f, g, c]

    def after_exchange(t0, slot):
        at = [step(t0 + j, states[j % 2], states[1 - j % 2]) for j in range(AHEAD)]
        late = [(state_a, half + q) for q in range(half - 3 * (half // 4))]
        for j in range(AHEAD):
            late = arc(at[j], halo + 1 + j, R - 2 * halo - 2 - 2 * j, 1, late)
        receive(1, slot)
        receive(0, slot)
        for r in (*range(halo), *range(R - halo, R)):
            edges(state_a, r)
        for j in range(AHEAD):
            late = arc(at[j], R - halo - 1 - j, 2 * halo + 2 + 2 * j, 1, late)
        for ref, r in late:
            edges(ref, r)

    def pair(i, _):
        level(2 * i, state_a, state_b)
        nth = (i + 1) * 2 // halo
        leave = (lax.rem(2 * i + 2, halo) == 0) & (2 * i + 2 < steps)

        @pl.when(i == 0)
        def _():
            convert(1)

        @pl.when(leave)
        def _():
            send(1, lax.rem(nth, 2))
        level(2 * i + 1, state_b, state_a)

        @pl.when(leave)
        def _():
            send(0, lax.rem(nth, 2))
        return 0

    phases = steps // halo

    def phase(p, _):
        @pl.when(p > 0)
        def _():
            after_exchange(p * halo, lax.rem(p, 2))
        lax.fori_loop(p * (halo // 2) + (p + phases - 1) // phases * (AHEAD // 2), (p + 1) * (halo // 2), pair, 0)
        return 0
    lax.fori_loop(0, phases, phase, 0)


def unpack_kernel(halo, a_ref, b_ref, u_hbm, v_hbm, raw, wide, sems):
    rows, cols = u_hbm.shape
    R = (rows + 2 * halo) // 8
    groups = [(r0, min(16, R - r0)) for r0 in range(0, R, 16)]
    copies = []
    for f, dst in enumerate((u_hbm, v_hbm)):
        for g, (r0, n) in enumerate(groups):
            for c in range(NC):
                parts = []
                for q in range(n):
                    at = pl.ds(((r0 + q) * NB + c + 1) * 8, 8)
                    if f == 0:
                        x = a_ref[at, :] * (1.0 / SCALE)
                    else:
                        x = (a_ref[at, :] - b_ref[at, :]) * (2.0 / SCALE)
                    parts.append(x)
                wide[f, g, pl.ds(c, 128, stride=NC), :8 * n] = jnp.concatenate(parts, axis=0).T
        for b in range(cols // 128):
            for g, (r0, n) in enumerate(groups):
                back = wide[f, g, pl.ds(b * 128, 128), :][:, :8 * n].T
                for q in range(n):
                    raw[f, b, pl.ds(r0 + q, 8, stride=R), :] = back[q * 8:q * 8 + 8, :]
            copies.append(pltpu.make_async_copy(raw.at[f, b, pl.ds(halo, rows), :], dst.at[:, pl.ds(b * 128, 128)],
                                                sems.at[f, b]))
            if len(copies) > 1:
                copies[-2].start()
    copies[-1].start()
    for cp in copies:
        cp.wait()


def solution(mesh):
    tile_spec = P(("ens", "row"), "col")

    def local_run(u_tile, v_tile, stencil_w):
        rows, cols = u_tile.shape
        steps = stencil_w.shape[0]
        halo = HALO
        R = (rows + 2 * halo) // 8
        nblk = cols // 128
        f32 = jnp.float32
        dma = pltpu.SemaphoreType.DMA
        raw = pltpu.VMEM((2, nblk + 1, 8 * R, 128), f32)
        wide = pltpu.VMEM((2, -(-R // 16), 128 * NC, 128), f32)
        vmem, hbm = pl.BlockSpec(memory_space=pltpu.VMEM), pl.BlockSpec(memory_space=pl.ANY)
        states = pl.pallas_call(
            functools.partial(kernel, steps, rows, cols, halo),
            out_shape=[jax.ShapeDtypeStruct((R * NB * 8, 128), f32)] * 2,
            in_specs=[hbm, hbm, hbm],
            out_specs=[vmem, vmem],
            scratch_shapes=[
                raw, pltpu.VMEM((2, rows, 128), f32), pltpu.VMEM((3, 3, steps), f32), pltpu.VMEM((5, steps, 128), f32), wide,
                pltpu.VMEM((2, 2, 2, halo // 8, NC, 8, 128), f32), pltpu.VMEM((2, 2, 2, halo // 8, NC, 8, 128), f32),
                dma((2, nblk)), dma((2, 2)), dma((2, 2, 2)), dma((2, 2, 2)), dma((2, 2, 2)), dma((2, 2, 2)), dma,
            ],
            compiler_params=pltpu.CompilerParams(collective_id=0, has_side_effects=True,
                                                 vmem_limit_bytes=44 * 1024 * 1024),
        )(*(pltpu.with_memory_space_constraint(x, pltpu.HBM) for x in (stencil_w.transpose(1, 2, 0), u_tile, v_tile)))
        return pl.pallas_call(
            functools.partial(unpack_kernel, halo),
            out_shape=[jax.ShapeDtypeStruct((rows, cols), f32)] * 2,
            in_specs=[vmem, vmem],
            out_specs=[hbm, hbm],
            scratch_shapes=[raw, wide, dma((2, nblk))],
            compiler_params=pltpu.CompilerParams(vmem_limit_bytes=32 * 1024 * 1024),
        )(*states)

    return jax.shard_map(local_run, mesh=mesh, in_specs=(tile_spec, tile_spec, P()), out_specs=(tile_spec, tile_spec), check_vma=False)
```
